256 devices in a mesh: seq: 32 (over y, x, core), tp: 8 (over z).
Axes of the slice: x: 4, y: 4, z: 8, core: 2. Of those that a mesh axis runs over, the one named last changes fastest.
Arguments:
- hidden_in: bfloat16 [2, 16384, 2560], P(None, 'seq'), may hold values from -6 to 6
- gate_proj: bfloat16 [2560, 5120], P(None, 'tp'), may hold values from -0.125 to 0.125
- value_proj: bfloat16 [2560, 5120], P(None, 'tp'), may hold values from -0.125 to 0.125
- bc_proj: bfloat16 [2560, 256], P(None, 'tp'), may hold values from -0.125 to 0.125
- step_proj: bfloat16 [2560, 80], P(None, 'tp'), may hold values from -0.125 to 0.125
- value_conv: float32 [4, 5120], P(None, 'tp'), may hold values from -3 to 3
- bc_conv: float32 [4, 256], replicated, may hold values from -3 to 3
- step_bias: float32 [80], P('tp'), may hold values from -1.5 to 0
- log_rate: float32 [80], P('tp'), as said below
- norm_gain: float32 [5120], P('tp'), may hold values from 0.25 to 1.75
Outputs:
- mixer_out: bfloat16 [2, 16384, 5120], P(None, 'seq', 'tp')
The draws below stay inside these ranges and needn't reach their ends.
Inputs may be any that keep to these rules, and one draw needn't show every extreme that they name: log_rate lies between -1.5 - ln(16384) and 1.0 - ln(16384).
All inputs are finite; a program needn't handle non-finite values.
Results may differ from the reference program's by a relative error of at most 0.0095.
Values may be sent and summed in bfloat16 or wider, within the bound.
No kernel may reach another device: no remote copies, remote signals or barrier semaphores. Data moves between devices by JAX's collectives and lax.ppermute only.
A program may use at most 128 MiB of HBM per device.

```python
import math
import jax
import jax.numpy as jnp
from jax import lax

D = 2560
DI = 5120
HEADS = 80
HEAD_DIM = 64
STATE = 128
CONV = 4
BATCH = 2
BLOCK = 64
SEQ_LEN = 16384


def draw_log_rate(key, part):
    shift = math.log(SEQ_LEN)
    return jax.random.uniform(key, (HEADS,), jnp.float32, -1.5 - shift, 1.0 - shift)


def level_of(own_key, dims, cuts, smallest, top_value):
    def one(axis_at, blocks):
        draws = jax.random.uniform(jax.random.fold_in(jax.random.fold_in(own_key, 6), axis_at), (blocks,), jnp.float32, smallest / len(cuts), top_value / len(cuts))
        return jnp.repeat(jnp.exp(draws), dims[axis_at] // blocks).reshape((-1,) + (1,) * (len(dims) - axis_at - 1))

    level = one(*cuts[0])
    for cut in cuts[1:]:
        level = level * one(*cut)
    return level


def noise(rng, extent, deviation, reach, shards=(), kind=jnp.bfloat16):
    entries = deviation * jax.random.normal(rng, extent, jnp.float32)
    if shards:
        entries = entries * level_of(rng, extent, shards, -0.22, 0.18)
    return jnp.clip(entries, -reach, reach).astype(kind)


def setup_inputs(seed: int = 0) -> dict:
    streams_of = jax.random.split(jax.random.key(seed), 11)
    hidden_in = noise(streams_of[0], (BATCH, SEQ_LEN, D), 1.0, 6.0, ((1, 32),))
    gate_proj = noise(streams_of[1], (D, DI), D ** -0.5, 0.125, ((1, 8),))
    value_proj = noise(streams_of[2], (D, DI), D ** -0.5, 0.125, ((1, 8),))
    bc_proj = noise(streams_of[3], (D, 2 * STATE), D ** -0.5, 0.125, ((1, 8),))
    step_proj = noise(streams_of[4], (D, HEADS), D ** -0.5, 0.125, ((1, 8),))
    value_conv = noise(streams_of[5], (CONV, DI), CONV ** -0.5, 3.0, ((1, 8),), jnp.float32)
    bc_conv = noise(streams_of[6], (CONV, 2 * STATE), CONV ** -0.5, 3.0, (), jnp.float32)
    step_bias = jnp.clip(-1.5 + 1.5 * jax.random.uniform(streams_of[7], (HEADS,), jnp.float32) ** level_of(streams_of[7], (HEADS,), ((0, 8),), -0.2, 0.2), -1.5, 0.0)
    log_rate = draw_log_rate(jax.random.fold_in(streams_of[10], 71), 0)
    norm_gain = jnp.clip(1.0 + 0.15 * jax.random.normal(streams_of[9], (DI,), jnp.float32), 0.25, 1.75)
    return {"hidden_in": hidden_in, "gate_proj": gate_proj, "value_proj": value_proj, "bc_proj": bc_proj, "step_proj": step_proj, "value_conv": value_conv, "bc_conv": bc_conv, "step_bias": step_bias, "log_rate": log_rate, "norm_gain": norm_gain}


epsilon = 1e-05

def conv_silu(padded, kernel, length):
    running = jnp.zeros((padded.shape[0], length, padded.shape[2]), jnp.float32)
    for tap_index in range(kernel.shape[0]):
        running = running + kernel[tap_index] * padded[:, tap_index:tap_index + length, :]
    return jax.nn.silu(running)

def block_step(carried, inputs):
    values, log_decay, step_sizes, b_rows, c_rows = inputs
    length = log_decay.shape[1]
    cumulative = jnp.cumsum(log_decay, axis=1)
    log_gap = cumulative[:, :, None, :] - cumulative[:, None, :, :]
    causal = jnp.arange(length)[:, None] >= jnp.arange(length)[None, :]
    weights_in = jnp.exp(jnp.where(causal[None, :, :, None], log_gap, -jnp.inf))
    scores = jnp.einsum('bin,bjn->bij', c_rows, b_rows, precision=lax.Precision.HIGHEST)
    mixing = scores[:, :, :, None] * weights_in * step_sizes[:, None, :, :]
    within = jnp.einsum('bijh,bjhp->bihp', mixing, values, precision=lax.Precision.HIGHEST)
    earlier = jnp.einsum('bin,bhpn->bihp', c_rows, carried, precision=lax.Precision.HIGHEST)
    earlier = earlier * jnp.exp(cumulative)[..., None]
    remain = jnp.exp(cumulative[:, -1:, :] - cumulative) * step_sizes
    added_state = jnp.einsum('bjh,bjhp,bjn->bhpn', remain, values, b_rows, precision=lax.Precision.HIGHEST)
    updated = jnp.exp(cumulative[:, -1, :])[:, :, None, None] * carried + added_state
    return (updated, within + earlier)

def to_blocks(series, batch_size, blocks):
    return jnp.moveaxis(series.reshape((batch_size, blocks, BLOCK) + series.shape[2:]), 1, 0)

def reference(hidden_in, gate_proj, value_proj, bc_proj, step_proj, value_conv, bc_conv, step_bias, log_rate, norm_gain):
    flat_rows = hidden_in.reshape(-1, D)
    gate_pre = jnp.dot(flat_rows, gate_proj, preferred_element_type=jnp.float32).astype(jnp.bfloat16)
    value_pre = jnp.dot(flat_rows, value_proj, preferred_element_type=jnp.float32).astype(jnp.bfloat16)
    bc_pre = jnp.dot(flat_rows, bc_proj, preferred_element_type=jnp.float32).astype(jnp.bfloat16)
    step_pre = jnp.dot(flat_rows, step_proj, preferred_element_type=jnp.float32)
    value_pad = jnp.pad(value_pre.reshape(BATCH, SEQ_LEN, DI).astype(jnp.float32), ((0, 0), (CONV - 1, 0), (0, 0)))
    bc_pad = jnp.pad(bc_pre.reshape(BATCH, SEQ_LEN, 2 * STATE).astype(jnp.float32), ((0, 0), (CONV - 1, 0), (0, 0)))
    values = conv_silu(value_pad, value_conv, SEQ_LEN).reshape(BATCH, SEQ_LEN, HEADS, HEAD_DIM)
    bc_rows = conv_silu(bc_pad, bc_conv, SEQ_LEN)
    b_rows = bc_rows[..., :STATE]
    c_rows = bc_rows[..., STATE:]
    step_sizes = jax.nn.softplus(step_pre.reshape(BATCH, SEQ_LEN, HEADS) + step_bias)
    log_decay = -step_sizes * jnp.exp(log_rate)
    blocks = SEQ_LEN // BLOCK
    initial = jnp.zeros((BATCH, HEADS, HEAD_DIM, STATE), jnp.float32)
    final_state, outputs = lax.scan(block_step, initial, (to_blocks(values, BATCH, blocks), to_blocks(log_decay, BATCH, blocks), to_blocks(step_sizes, BATCH, blocks), to_blocks(b_rows, BATCH, blocks), to_blocks(c_rows, BATCH, blocks)))
    mixed_out = jnp.moveaxis(outputs, 0, 1).reshape(BATCH, SEQ_LEN, DI)
    gated_out = mixed_out * jax.nn.silu(gate_pre.reshape(BATCH, SEQ_LEN, DI).astype(jnp.float32))
    scale_sq = lax.optimization_barrier(jnp.sum(gated_out * gated_out, axis=-1, keepdims=True)) / DI
    return (gated_out * lax.rsqrt(scale_sq + epsilon) * norm_gain).astype(jnp.bfloat16)
```

```python
import functools

import jax
import jax.numpy as jnp
from jax import lax
from jax.experimental import pallas as pl
from jax.experimental.pallas import tpu as pltpu
from jax.sharding import Mesh
from jax.sharding import PartitionSpec as P

DI = 5120
HEAD_DIM = 64
STATE = 128
CONV = 4
BLOCK = 128
LANES = 128
EPSILON = 1e-05

F32 = jnp.float32
BF16 = jnp.bfloat16
HIGHEST = lax.Precision.HIGHEST
NT = (((1,), (1,)), ((), ()))


def dot(a, b):
    return jnp.dot(a, b, preferred_element_type=F32)


def dot_nt(a, b):
    return lax.dot_general(a, b, NT, preferred_element_type=F32)


def silu(x):
    return x / (1.0 + jnp.exp(-x))


def split_in_three(x):
    high = x.astype(BF16)
    rest = x - high.astype(F32)
    middle = rest.astype(BF16)
    return high, middle, (rest - middle.astype(F32)).astype(BF16)


def head_lanes(width):
    head = lax.broadcasted_iota(jnp.int32, (LANES, width), 1) // HEAD_DIM
    row = lax.broadcasted_iota(jnp.int32, (LANES, width), 0)
    return (head == row).astype(BF16)


def over_channels(x, spread):
    high, middle, low = split_in_three(x)
    return dot(high, spread) + dot(middle, spread) + dot(low, spread)


def bc_kernel(batch, length, hidden, halo, weight, out, pad):
    share = weight.shape[0]
    pad[...] = jnp.zeros_like(pad)
    before = dot_nt(halo[...], weight[...])
    for b in range(batch):
        pad[LANES - 8 - 64 * b : LANES - 64 * b, :share] = before[8 * b : 8 * b + 8]
    tile = jnp.transpose(pad[...])[:share].astype(BF16)
    for d in range(out.shape[0]):
        out[d, :, :LANES] = tile
    for j in range(batch * length // LANES):
        part = dot_nt(hidden[j * LANES : (j + 1) * LANES, :], weight[...])
        pad[:, :share] = part
        tile = jnp.transpose(pad[...])[:share].astype(BF16)
        for d in range(out.shape[0]):
            out[d, :, (j + 1) * LANES : (j + 2) * LANES] = tile


def value_kernel(
    batch, length, hidden, halo, weight, taps, step_weight, step_bias, log_rate,
    scaled, opening, rows, decays, padded,
):
    inner = weight.shape[1]
    blocks = length // BLOCK
    spread = head_lanes(inner)
    before = dot(halo[...], weight[...]).astype(BF16).astype(F32)
    rate = jnp.exp(log_rate[0:1, :])
    i = lax.broadcasted_iota(jnp.int32, (BLOCK, BLOCK), 0)
    j = lax.broadcasted_iota(jnp.int32, (BLOCK, BLOCK), 1)
    lower = (i >= j).astype(BF16)
    halves, offsets = [], []
    for b in range(batch):
        own = hidden[b * length : (b + 1) * length, :]
        padded[0:8, :] = before[8 * b : 8 * b + 8]
        padded[8 : 8 + length, :] = dot(own, weight[...]).astype(BF16).astype(F32)
        step_pre = dot_nt(own, step_weight[...]) + step_bias[0:1, :]
        steps = jnp.maximum(step_pre, 0.0) + jnp.log1p(jnp.exp(-jnp.abs(step_pre)))
        total = jnp.zeros((1, LANES), F32)
        for k in range(blocks):
            r = k * BLOCK
            step = steps[r : r + BLOCK]
            high, middle, low = split_in_three(-step * rate)
            cumulative = dot(lower, high) + dot(lower, middle) + dot(lower, low)
            last = cumulative[BLOCK - 1 : BLOCK, :]
            centered = cumulative - 0.5 * last
            halves.append(0.5 * last)
            offsets.append(total + 0.5 * last)
            total = total + last
            value = sum(
                taps[t : t + 1, :] * padded[r + 5 + t : r + 5 + t + BLOCK, :] for t in range(CONV)
            )
            ahead = over_channels(jnp.exp(-centered) * step, spread)
            at = b * length + r
            scaled[at : at + BLOCK, :] = (silu(value) * ahead).astype(BF16)
            opening[at : at + BLOCK, :] = jnp.exp(centered)
        high, middle, low = split_in_three(total)
        decays[b] = jnp.concatenate(
            [high, middle, low, jnp.zeros((5, LANES), BF16)], axis=0
        )
    rows[...] = jnp.exp(over_channels(jnp.concatenate(halves + offsets, axis=0), spread))


def gate_kernel(batch, length, hidden, weight, opening, out):
    spread = head_lanes(weight.shape[1])
    for b in range(batch):
        at = slice(b * length, (b + 1) * length)
        gate = dot(hidden[at, :], weight[...]).astype(BF16).astype(F32)
        out[at, :] = (silu(gate) * over_channels(opening[at, :], spread)).astype(BF16)


def state_kernel(batch, length, bc, taps, scaled, rows, decays, b_rows, c_rows, starts, sent):
    blocks = length // BLOCK
    inner = scaled.shape[1]
    halo = bc[:, :LANES].astype(F32)
    for b in range(batch):
        own = bc[:, LANES + b * length : LANES + (b + 1) * length].astype(F32)
        before = pltpu.roll(halo, 64 * b, 1) if b else halo
        padded = jnp.concatenate([before, own], axis=1)
        mixed = taps[:, CONV - 1 : CONV] * own
        for t in range(CONV - 1):
            mixed = mixed + taps[:, t : t + 1] * pltpu.roll(padded, CONV - 1 - t, 1)[:, LANES:]
        mixed = silu(mixed)
        b_t = mixed[:STATE].astype(BF16)
        b_rows[b] = b_t
        c_rows[b * length : (b + 1) * length, :] = jnp.transpose(mixed[STATE:]).astype(BF16)
        state = jnp.zeros((STATE, inner), F32)
        for k in range(blocks):
            n = b * blocks + k
            half = rows[n : n + 1, :]
            ready = half * state
            starts[n] = ready.astype(BF16)
            at = b * length + k * BLOCK
            added = dot(b_t[:, k * BLOCK : (k + 1) * BLOCK], scaled[at : at + BLOCK, :])
            state = half * (ready + added)
        for g in range(STATE // 8):
            sent[b, g, :, :inner] = state[8 * g : 8 * g + 8].astype(BF16)
            sent[b, g, :, inner:] = decays[b]


def within_kernel(batch, length, b_rows, c_rows, scaled, starts, out):
    blocks = length // BLOCK
    i = lax.broadcasted_iota(jnp.int32, (BLOCK, BLOCK), 0)
    j = lax.broadcasted_iota(jnp.int32, (BLOCK, BLOCK), 1)
    for b in range(batch):
        for k in range(blocks):
            at = slice(b * length + k * BLOCK, b * length + (k + 1) * BLOCK)
            c = c_rows[at, :]
            scores = dot(c, b_rows[b, :, k * BLOCK : (k + 1) * BLOCK])
            scores = jnp.where(i >= j, scores, 0.0).astype(BF16)
            out[at, :] = dot(scores, scaled[at, :]) + dot(c, starts[b * blocks + k])


def scan_kernel(got, out, table, logs):
    devices, _, width = got.shape
    inner = width - LANES
    for s in range(devices):
        parts = got[s, :, inner:].astype(F32)
        table[s : s + 1, :] = parts[0:1] + parts[1:2] + parts[2:3]
    logs[...] = jnp.exp(over_channels(table[...], head_lanes(inner)))
    state = jnp.zeros((8, inner), F32)
    for s in range(devices):
        out[s] = state.astype(BF16)
        state = logs[s : s + 1, :] * state + got[s, :, :inner].astype(F32)


def gated_kernel(batch, length, c_rows, arrived, within, opened, rows, gated, squares):
    blocks = length // BLOCK
    count = batch * blocks
    inner = within.shape[1]
    ones = jnp.ones((8, inner), BF16)
    for b in range(batch):
        for k in range(blocks):
            n = b * blocks + k
            at = slice(n * BLOCK, (n + 1) * BLOCK)
            late = dot(c_rows[at, :], arrived[b])
            y = within[at, :] + rows[count + n : count + n + 1, :] * late
            g = y * opened[at, :].astype(F32)
            gated[at, :] = g
            squares[:, n, :] = dot_nt(ones, (g * g).astype(BF16))


def scale_kernel(gated, squares, gain, out):
    total = squares[0]
    for d in range(1, squares.shape[0]):
        total = total + squares[d]
    scale = lax.rsqrt(total / DI + EPSILON)
    count = scale.shape[0]
    scale = jnp.concatenate([scale, jnp.zeros((LANES - count, LANES), F32)], axis=0)
    columns = jnp.transpose(scale)
    for n in range(count):
        at = slice(n * LANES, (n + 1) * LANES)
        out[at, :] = (gated[at, :] * columns[:, n : n + 1] * gain[0:1, :]).astype(BF16)


def call(kernel, out, scratch=(), mib=28, flops=0):
    shapes = [jax.ShapeDtypeStruct(s, d) for s, d in out]
    return pl.pallas_call(
        kernel,
        out_shape=shapes if len(shapes) > 1 else shapes[0],
        scratch_shapes=[pltpu.VMEM(s, d) for s, d in scratch],
        compiler_params=pltpu.CompilerParams(vmem_limit_bytes=mib << 20),
        cost_estimate=pl.CostEstimate(flops=flops, transcendentals=0, bytes_accessed=0)
        if flops
        else None,
    )


def on_device(
    hidden_in, gate_proj, value_proj, bc_proj, step_proj, value_conv, bc_conv, step_bias, log_rate,
    norm_gain,
):
    batch, length, width = hidden_in.shape
    tokens = batch * length
    inner = value_proj.shape[1]
    heads = step_proj.shape[1]
    share = bc_proj.shape[1]
    states = 2 * STATE
    blocks = tokens // BLOCK
    seq, tp = lax.axis_size("seq"), lax.axis_size("tp")
    hidden = hidden_in.reshape(tokens, width)
    tail = hidden_in[:, length - 8 :, :]
    halo = lax.ppermute(tail, "seq", [(i, i + 1) for i in range(seq - 1)]).reshape(8 * batch, width)
    bc_part = call(
        functools.partial(bc_kernel, batch, length),
        [((tp, share, tokens + LANES), BF16)],
        [((LANES, LANES), F32)],
    )(hidden, halo, bc_proj.T)
    bc = lax.all_to_all(bc_part, "tp", 0, 0, tiled=True).reshape(states, tokens + LANES)
    lane = jnp.pad
    scaled, opening, rows, decays = call(
        functools.partial(value_kernel, batch, length),
        [
            ((tokens, inner), BF16),
            ((tokens, LANES), F32),
            ((2 * blocks, inner), F32),
            ((batch, 8, LANES), BF16),
        ],
        [((length + 8, inner), F32)],
        flops=2 * tokens * width * inner,
    )(
        hidden,
        halo,
        value_proj,
        value_conv,
        lane(step_proj.T, ((0, LANES - heads), (0, 0))),
        lane(step_bias, (0, LANES - heads)).reshape(1, LANES),
        lane(log_rate, (0, LANES - heads), constant_values=-1e30).reshape(1, LANES),
    )
    opened = call(
        functools.partial(gate_kernel, batch, length),
        [((tokens, inner), BF16)],
        flops=2 * tokens * width * inner,
    )(hidden, gate_proj, opening)
    b_rows, c_rows, starts, sent = call(
        functools.partial(state_kernel, batch, length),
        [
            ((batch, STATE, length), BF16),
            ((tokens, STATE), BF16),
            ((blocks, STATE, inner), BF16),
            ((batch, STATE // 8, 8, inner + LANES), BF16),
        ],
    )(bc, bc_conv.T, scaled, rows, decays)
    got = lax.all_to_all(sent.reshape(seq, -1, inner + LANES), "seq", 0, 0, tiled=True)
    within = call(
        functools.partial(within_kernel, batch, length),
        [((tokens, inner), F32)],
        flops=2 * tokens * width * inner // 4,
    )(b_rows, c_rows, scaled, starts)
    prefix = call(
        scan_kernel,
        [((seq, 8, inner), BF16)],
        [((seq, LANES), F32), ((seq, inner), F32)],
    )(got)
    arrived = lax.all_to_all(prefix, "seq", 0, 0, tiled=True).reshape(batch, STATE, inner)
    gated, squares = call(
        functools.partial(gated_kernel, batch, length),
        [((tokens, inner), F32), ((tp, blocks, LANES), F32)],
    )(c_rows, arrived, within, opened, rows)
    whole = lax.all_to_all(squares, "tp", 0, 0, tiled=True)
    out = call(scale_kernel, [((tokens, inner), BF16)])(gated, whole, norm_gain.reshape(1, inner))
    return out.reshape(batch, length, inner)


def solution(mesh):
    placed = (
        P(None, "seq", None),
        P(None, "tp"),
        P(None, "tp"),
        P(None, "tp"),
        P(None, "tp"),
        P(None, "tp"),
        P(),
        P("tp"),
        P("tp"),
        P("tp"),
    )
    return jax.shard_map(
        on_device, mesh=mesh, in_specs=placed, out_specs=P(None, "seq", "tp"), check_vma=False
    )
```

```python
import functools

import jax
import jax.numpy as jnp
from jax import lax
from jax.experimental import pallas as pl
from jax.experimental.pallas import tpu as pltpu
from jax.sharding import Mesh
from jax.sharding import PartitionSpec as P

DI = 5120
HEAD_DIM = 64
STATE = 128
CONV = 4
BLOCK = 128
LANES = 128
EPSILON = 1e-05

F32 = jnp.float32
BF16 = jnp.bfloat16
HIGHEST = lax.Precision.HIGHEST
NT = (((1,), (1,)), ((), ()))


def dot(a, b):
    return jnp.dot(a, b, preferred_element_type=F32)


def dot_nt(a, b):
    return lax.dot_general(a, b, NT, preferred_element_type=F32)


def silu(x):
    return x / (1.0 + jnp.exp(-x))


def split_in_three(x):
    high = x.astype(BF16)
    rest = x - high.astype(F32)
    middle = rest.astype(BF16)
    return high, middle, (rest - middle.astype(F32)).astype(BF16)


def head_lanes(width):
    head = lax.broadcasted_iota(jnp.int32, (LANES, width), 1) // HEAD_DIM
    row = lax.broadcasted_iota(jnp.int32, (LANES, width), 0)
    return (head == row).astype(BF16)


def over_channels(x, spread):
    high, middle, low = split_in_three(x)
    return dot(high, spread) + dot(middle, spread) + dot(low, spread)


def transposed(part, pad):
    pad[:, : part.shape[1]] = part
    return jnp.transpose(pad[...])[: part.shape[1]].astype(BF16)


def bc_kernel(hidden, weight, out, pad):
    pad[...] = jnp.zeros_like(pad)
    out[...] = transposed(dot_nt(hidden[...], weight[...]), pad)


def join_kernel(batch, halo, weight, own, out, pad):
    share = weight.shape[0]
    before = dot_nt(halo[...], weight[...])
    pad[...] = jnp.zeros_like(pad)
    for b in range(batch):
        pad[LANES - 8 - 64 * b : LANES - 64 * b, :share] = before[8 * b : 8 * b + 8]
    tile = jnp.transpose(pad[...])[:share].astype(BF16)
    for d in range(out.shape[0]):
        out[d, :, :LANES] = tile
        out[d, :, LANES:] = own[...]


def project_kernel(
    batch, length, chunk, hidden, value_weight, gate_weight, halo, taps, step_weight, step_bias,
    log_rate, gain, scaled, opened, rows, decays, hid, vw, gw, padded, scaled_v, opened_v, sems,
):
    inner = vw.shape[1]
    tokens = batch * length
    chunks = tokens // chunk
    spread = head_lanes(inner)

    def fetch(c):
        at = pl.ds(c * chunk, chunk)
        return pltpu.make_async_copy(hidden.at[at, :], hid.at[at, :], sems.at[c])

    def store(c, source, target, k):
        at = pl.ds(c * chunk, chunk)
        return pltpu.make_async_copy(source.at[at, :], target.at[at, :], sems.at[k * chunks + 2 + c])

    value_copy = pltpu.make_async_copy(value_weight, vw, sems.at[chunks])
    gate_copy = pltpu.make_async_copy(gate_weight, gw, sems.at[chunks + 1])
    value_copy.start()
    fetch(0).start()
    rate = jnp.exp(log_rate[0:1, :])
    i = lax.broadcasted_iota(jnp.int32, (BLOCK, BLOCK), 0)
    j = lax.broadcasted_iota(jnp.int32, (BLOCK, BLOCK), 1)
    lower = (i >= j).astype(BF16)
    halves, offsets = [], []
    fetch(0).wait()
    value_copy.wait()
    for c in range(1, chunks):
        fetch(c).start()
    gate_copy.start()
    before = dot(halo[...], vw[...]).astype(BF16).astype(F32)
    for c in range(chunks):
        at = slice(c * chunk, (c + 1) * chunk)
        b = c * chunk // length
        if c:
            fetch(c).wait()
        own = hid[at, :]
        if c * chunk % length == 0:
            padded[0:8, :] = before[8 * b : 8 * b + 8]
            total = jnp.zeros((1, LANES), F32)
        else:
            padded[0:8, :] = padded[chunk : chunk + 8, :]
        padded[8 : 8 + chunk, :] = dot(own, vw[...]).astype(BF16).astype(F32)
        step_pre = dot_nt(own, step_weight[...]) + step_bias[0:1, :]
        steps = jnp.maximum(step_pre, 0.0) + jnp.log1p(jnp.exp(-jnp.abs(step_pre)))
        opening = []
        for r in range(0, chunk, BLOCK):
            step = steps[r : r + BLOCK]
            high, middle, low = split_in_three(-step * rate)
            cumulative = dot(lower, high) + dot(lower, middle) + dot(lower, low)
            last = cumulative[BLOCK - 1 : BLOCK, :]
            centered = cumulative - 0.5 * last
            halves.append(0.5 * last)
            offsets.append(total + 0.5 * last)
            total = total + last
            value = sum(
                taps[t : t + 1, :] * padded[r + 5 + t : r + 5 + t + BLOCK, :] for t in range(CONV)
            )
            ahead = over_channels(jnp.exp(-centered) * step, spread)
            scaled_v[c * chunk + r : c * chunk + r + BLOCK, :] = (silu(value) * ahead).astype(BF16)
            opening.append(jnp.exp(centered))
        store(c, scaled_v, scaled, 1).start()
        if (c + 1) * chunk % length == 0:
            high, middle, low = split_in_three(total)
            decays[b] = jnp.concatenate([high, middle, low, jnp.zeros((5, LANES), BF16)], axis=0)
        if c == 0:
            gate_copy.wait()
        gate = dot(own, gw[...]).astype(BF16).astype(F32)
        behind = over_channels(jnp.concatenate(opening, axis=0), spread)
        opened_v[at, :] = (silu(gate) * behind).astype(BF16)
        store(c, opened_v, opened, 2).start()
    count = len(halves) + len(offsets)
    rows[:count, :] = jnp.exp(over_channels(jnp.concatenate(halves + offsets, axis=0), spread))
    rows[count:, :] = jnp.concatenate([gain[0:1, :]] * (rows.shape[0] - count), axis=0)
    for c in range(chunks):
        store(c, scaled_v, scaled, 1).wait()
        store(c, opened_v, opened, 2).wait()


def state_kernel(batch, length, bc, taps, scaled, rows, decays, b_rows, c_rows, starts, sent):
    blocks = length // BLOCK
    inner = scaled.shape[1]
    halo = bc[:, :LANES].astype(F32)
    for b in range(batch):
        own = bc[:, LANES + b * length : LANES + (b + 1) * length].astype(F32)
        before = pltpu.roll(halo, 64 * b, 1) if b else halo
        padded = jnp.concatenate([before, own], axis=1)
        mixed = taps[:, CONV - 1 : CONV] * own
        for t in range(CONV - 1):
            mixed = mixed + taps[:, t : t + 1] * pltpu.roll(padded, CONV - 1 - t, 1)[:, LANES:]
        mixed = silu(mixed)
        b_t = mixed[:STATE].astype(BF16)
        b_rows[b] = b_t
        c_rows[b * length : (b + 1) * length, :] = jnp.transpose(mixed[STATE:]).astype(BF16)
        state = jnp.zeros((STATE, inner), F32)
        for k in range(blocks):
            n = b * blocks + k
            half = rows[n : n + 1, :]
            ready = half * state
            starts[n] = ready.astype(BF16)
            at = b * length + k * BLOCK
            added = dot(b_t[:, k * BLOCK : (k + 1) * BLOCK], scaled[at : at + BLOCK, :])
            state = half * (ready + added)
        for g in range(STATE // 8):
            sent[b, g, :, :inner] = state[8 * g : 8 * g + 8].astype(BF16)
            sent[b, g, :, inner:] = decays[b]


def scan_kernel(got, out, table, logs):
    devices, _, width = got.shape
    inner = width - LANES
    for s in range(devices):
        parts = got[s, :, inner:].astype(F32)
        table[s : s + 1, :] = parts[0:1] + parts[1:2] + parts[2:3]
    logs[...] = jnp.exp(over_channels(table[...], head_lanes(inner)))
    state = jnp.zeros((8, inner), F32)
    for s in range(devices):
        out[s] = state.astype(BF16)
        state = logs[s : s + 1, :] * state + got[s, :, :inner].astype(F32)


def gated_kernel(
    batch, length, arrived, b_rows, c_rows, scaled, starts, opened, rows, gated, squares
):
    blocks = length // BLOCK
    count = batch * blocks
    ones = jnp.ones((8, scaled.shape[1]), BF16)
    i = lax.broadcasted_iota(jnp.int32, (BLOCK, BLOCK), 0)
    j = lax.broadcasted_iota(jnp.int32, (BLOCK, BLOCK), 1)
    for b in range(batch):
        for k in range(blocks):
            n = b * blocks + k
            at = slice(n * BLOCK, (n + 1) * BLOCK)
            c = c_rows[at, :]
            scores = dot(c, b_rows[b, :, k * BLOCK : (k + 1) * BLOCK])
            scores = jnp.where(i >= j, scores, 0.0).astype(BF16)
            y = dot(scores, scaled[at, :]) + dot(c, starts[n])
            y = y + rows[count + n : count + n + 1, :] * dot(c, arrived[b])
            g = y * opened[at, :].astype(F32)
            gated[at, :] = g
            squares[:, n, :] = dot_nt(ones, (g * g).astype(BF16))


def scale_kernel(gated, squares, rows, out):
    total = squares[0]
    for d in range(1, squares.shape[0]):
        total = total + squares[d]
    scale = lax.rsqrt(total / DI + EPSILON)
    count = scale.shape[0]
    scale = jnp.concatenate([scale, jnp.zeros((LANES - count, LANES), F32)], axis=0)
    columns = jnp.transpose(scale)
    gain = rows[2 * count : 2 * count + 1, :]
    for n in range(count):
        at = slice(n * LANES, (n + 1) * LANES)
        out[at, :] = (gated[at, :] * columns[:, n : n + 1] * gain).astype(BF16)


ANY = pl.BlockSpec(memory_space=pl.ANY)
WHOLE = pl.BlockSpec(memory_space=pltpu.VMEM)


def call(kernel, out, ins=None, scratch=(), mib=12, flops=0, outs=None, grid=()):
    shapes = [jax.ShapeDtypeStruct(s, d) for s, d in out]
    specs = {} if ins is None else {"in_specs": ins}
    if outs is not None:
        specs["out_specs"] = outs if len(outs) > 1 else outs[0]
    return pl.pallas_call(
        kernel,
        out_shape=shapes if len(shapes) > 1 else shapes[0],
        grid=grid,
        scratch_shapes=[s if not isinstance(s, tuple) else pltpu.VMEM(*s) for s in scratch],
        compiler_params=pltpu.CompilerParams(vmem_limit_bytes=mib << 20),
        cost_estimate=pl.CostEstimate(flops=flops, transcendentals=0, bytes_accessed=0)
        if flops
        else None,
        **specs,
    )


def on_device(
    hidden_in, gate_proj, value_proj, bc_proj, step_proj, value_conv, bc_conv, step_bias, log_rate,
    norm_gain,
):
    batch, length, width = hidden_in.shape
    tokens = batch * length
    inner = value_proj.shape[1]
    heads = step_proj.shape[1]
    share = bc_proj.shape[1]
    states = 2 * STATE
    blocks = tokens // BLOCK
    seq, tp = lax.axis_size("seq"), lax.axis_size("tp")
    hidden = hidden_in.reshape(tokens, width)
    tail = hidden_in[:, length - 8 :, :]
    halo = lax.ppermute(tail, "seq", [(i, i + 1) for i in range(seq - 1)]).reshape(8 * batch, width)
    chunk = 256
    own = call(
        bc_kernel,
        [((share, tokens), BF16)],
        ins=[
            pl.BlockSpec((chunk, width), lambda c: (c, 0)),
            pl.BlockSpec((share, width), lambda c: (0, 0)),
        ],
        outs=[pl.BlockSpec((share, chunk), lambda c: (0, c))],
        scratch=[((chunk, LANES), F32)],
        grid=(tokens // chunk,),
        mib=60,
        flops=2 * tokens * width * share,
    )(hidden, bc_proj.T)
    bc_part = call(
        functools.partial(join_kernel, batch),
        [((tp, share, tokens + LANES), BF16)],
        scratch=[((LANES, LANES), F32)],
    )(halo, bc_proj.T, own)
    bc = lax.all_to_all(bc_part, "tp", 0, 0, tiled=True).reshape(states, tokens + LANES)
    scaled, opened, rows, decays = call(
        functools.partial(project_kernel, batch, length, chunk),
        [
            ((tokens, inner), BF16),
            ((tokens, inner), BF16),
            ((2 * blocks + 8, inner), F32),
            ((batch, 8, LANES), BF16),
        ],
        ins=[ANY, ANY, ANY] + [WHOLE] * 6,
        outs=[ANY, ANY, WHOLE, WHOLE],
        scratch=[
            ((tokens, width), BF16),
            ((width, inner), BF16),
            ((width, inner), BF16),
            ((chunk + 8, inner), F32),
            ((tokens, inner), BF16),
            ((tokens, inner), BF16),
            pltpu.SemaphoreType.DMA((3 * (tokens // chunk) + 2,)),
        ],
        mib=60,
        flops=4 * tokens * width * inner,
    )(
        hidden,
        value_proj,
        gate_proj,
        halo,
        value_conv,
        jnp.pad(step_proj.T, ((0, LANES - heads), (0, 0))),
        jnp.pad(step_bias, (0, LANES - heads)).reshape(1, LANES),
        jnp.pad(log_rate, (0, LANES - heads), constant_values=-1e30).reshape(1, LANES),
        norm_gain.reshape(1, inner),
    )
    b_rows, c_rows, starts, sent = call(
        functools.partial(state_kernel, batch, length),
        [
            ((batch, STATE, length), BF16),
            ((tokens, STATE), BF16),
            ((blocks, STATE, inner), BF16),
            ((batch, STATE // 8, 8, inner + LANES), BF16),
        ],
        mib=16,
    )(bc, bc_conv.T, scaled, rows, decays)
    got = lax.all_to_all(sent.reshape(seq, -1, inner + LANES), "seq", 0, 0, tiled=True)
    prefix = call(
        scan_kernel,
        [((seq, 8, inner), BF16)],
        scratch=[((seq, LANES), F32), ((seq, inner), F32)],
    )(got)
    arrived = lax.all_to_all(prefix, "seq", 0, 0, tiled=True).reshape(batch, STATE, inner)
    gated, squares = call(
        functools.partial(gated_kernel, batch, length),
        [((tokens, inner), F32), ((tp, blocks, LANES), F32)],
        mib=16,
    )(arrived, b_rows, c_rows, scaled, starts, opened, rows)
    whole = lax.all_to_all(squares, "tp", 0, 0, tiled=True)
    out = call(scale_kernel, [((tokens, inner), BF16)], mib=12)(gated, whole, rows)
    return out.reshape(batch, length, inner)


def solution(mesh):
    placed = (
        P(None, "seq", None),
        P(None, "tp"),
        P(None, "tp"),
        P(None, "tp"),
        P(None, "tp"),
        P(None, "tp"),
        P(),
        P("tp"),
        P("tp"),
        P("tp"),
    )
    return jax.shard_map(
        on_device, mesh=mesh, in_specs=placed, out_specs=P(None, "seq", "tp"), check_vma=False
    )
```

```python
import functools

import jax
import jax.numpy as jnp
from jax import lax
from jax.experimental import pallas as pl
from jax.experimental.pallas import tpu as pltpu
from jax.sharding import Mesh
from jax.sharding import PartitionSpec as P

DI = 5120
HEAD_DIM = 64
STATE = 128
CONV = 4
BLOCK = 128
LANES = 128
EPSILON = 1e-05

F32 = jnp.float32
BF16 = jnp.bfloat16
HIGHEST = lax.Precision.HIGHEST
NT = (((1,), (1,)), ((), ()))


def dot(a, b):
    return jnp.dot(a, b, preferred_element_type=F32)


def dot_nt(a, b):
    return lax.dot_general(a, b, NT, preferred_element_type=F32)


def silu(x):
    half = 0.5 * x
    return half + half * jnp.tanh(half)


def split_in_three(x):
    high = x.astype(BF16)
    rest = x - high.astype(F32)
    middle = rest.astype(BF16)
    return high, middle, (rest - middle.astype(F32)).astype(BF16)


def head_lanes(width):
    head = lax.broadcasted_iota(jnp.int32, (2 * LANES, width), 1) // HEAD_DIM
    row = lax.broadcasted_iota(jnp.int32, (2 * LANES, width), 0)
    return (head == lax.rem(row, LANES)).astype(BF16)


def over_channels(x, spread):
    high, middle, _ = split_in_three(x)
    return dot(jnp.concatenate([high, middle], axis=1), spread)


def transposed(part, pad):
    pad[:, : part.shape[1]] = part
    return jnp.transpose(pad[...])[: part.shape[1]].astype(BF16)


def bc_kernel(chunk, hidden, weight, out, pad):
    pad[...] = jnp.zeros_like(pad)
    for r in range(0, hidden.shape[0], chunk):
        part = dot_nt(hidden[r : r + chunk, :], weight[...])
        out[:, r : r + chunk] = transposed(part, pad)


def join_kernel(batch, halo, weight, own, out, pad):
    share = weight.shape[0]
    before = dot_nt(halo[...], weight[...])
    pad[...] = jnp.zeros_like(pad)
    for b in range(batch):
        pad[LANES - 8 - 64 * b : LANES - 64 * b, :share] = before[8 * b : 8 * b + 8]
    out[:, :LANES] = jnp.transpose(pad[...])[:share].astype(BF16)
    out[:, LANES:] = own[...]


def value_kernel(
    b, length, step_bias, log_rate, hidden, halo, weight, taps, step_weight,
    scaled, opening, rows, decays, padded, step_pad,
):
    inner = weight.shape[1]
    heads = step_weight.shape[0]
    spread = head_lanes(inner)
    step_pad[...] = jnp.zeros_like(step_pad)
    step_pad[:heads, :] = step_weight[...]
    lane = lax.broadcasted_iota(jnp.int32, (1, LANES), 1)
    bias, rate = jnp.zeros((1, LANES), F32), jnp.full((1, LANES), -1e30, F32)
    for h in range(heads):
        bias = jnp.where(lane == h, step_bias[h], bias)
        rate = jnp.where(lane == h, log_rate[h], rate)
    rate = jnp.exp(rate)
    own = hidden[b * length : (b + 1) * length, :]
    before = dot(halo[...], weight[...]).astype(BF16).astype(F32)
    padded[0:8, :] = before[8 * b : 8 * b + 8]
    padded[8 : 8 + length, :] = dot(own, weight[...]).astype(BF16).astype(F32)
    step_pre = dot_nt(own, step_pad[...]) + bias
    steps = jnp.maximum(step_pre, 0.0) + jnp.log1p(jnp.exp(-jnp.abs(step_pre)))
    i = lax.broadcasted_iota(jnp.int32, (BLOCK, BLOCK), 0)
    j = lax.broadcasted_iota(jnp.int32, (BLOCK, BLOCK), 1)
    lower = (i >= j).astype(BF16)
    total = jnp.zeros((1, LANES), F32)
    halves, offsets = [], []
    for r in range(0, length, BLOCK):
        step = steps[r : r + BLOCK]
        high, middle, low = split_in_three(-step * rate)
        cumulative = dot(lower, high) + dot(lower, middle) + dot(lower, low)
        last = cumulative[BLOCK - 1 : BLOCK, :]
        centered = cumulative - 0.5 * last
        halves.append(0.5 * last)
        offsets.append(total + 0.5 * last)
        total = total + last
        value = sum(taps[t : t + 1, :] * padded[r + 5 + t : r + 5 + t + BLOCK, :] for t in range(CONV))
        ahead = over_channels(jnp.exp(-centered) * step, spread)
        scaled[r : r + BLOCK, :] = (silu(value) * ahead).astype(BF16)
        opening[r : r + BLOCK, :] = jnp.exp(centered)
    high, middle, low = split_in_three(total)
    decays[...] = jnp.concatenate([high, middle, low, jnp.zeros((5, LANES), BF16)], axis=0)
    rows[...] = jnp.exp(over_channels(jnp.concatenate(halves + offsets, axis=0), spread))


def gate_kernel(b, length, hidden, weight, opening, out):
    gate = dot(hidden[b * length : (b + 1) * length, :], weight[...]).astype(BF16).astype(F32)
    out[...] = (silu(gate) * over_channels(opening[...], head_lanes(weight.shape[1]))).astype(BF16)


def state_kernel(batch, length, steps, place, taps, *refs):
    shards, refs = refs[: len(steps)], refs[len(steps) :]
    scaled, refs = refs[:batch], refs[batch:]
    rows, refs = refs[:batch], refs[batch:]
    decays, (b_rows, c_rows, starts, sent, mixed, columns) = refs[:batch], refs[batch:]
    blocks = length // BLOCK
    inner = scaled[0].shape[1]
    share = shards[0].shape[0]
    rest = jnp.zeros((LANES - CONV, 2 * STATE), F32)
    columns[...] = jnp.transpose(jnp.concatenate([taps[...], rest], axis=0))
    for step, shard in zip(steps, shards):
        first = pl.multiple_of(lax.rem(place[0] + step, len(steps)) * share, share)
        tap = columns[pl.ds(first, share), :]
        halo = shard[:, :LANES].astype(F32)
        for b in range(batch):
            own = shard[:, LANES + b * length : LANES + (b + 1) * length].astype(F32)
            before = pltpu.roll(halo, 64 * b, 1) if b else halo
            padded = jnp.concatenate([before, own], axis=1)
            total = tap[:, CONV - 1 : CONV] * own
            for t in range(CONV - 1):
                total = total + tap[:, t : t + 1] * pltpu.roll(padded, CONV - 1 - t, 1)[:, LANES:]
            mixed[pl.ds(first, share), b * length : (b + 1) * length] = silu(total)
    for b in range(batch):
        own = slice(b * length, (b + 1) * length)
        b_t = mixed[:STATE, own].astype(BF16)
        b_rows[b] = b_t
        c_rows[own, :] = jnp.transpose(mixed[STATE:, own]).astype(BF16)
        state = jnp.zeros((STATE, inner), F32)
        for k in range(blocks):
            half = rows[b][k : k + 1, :]
            ready = half * state
            starts[b * blocks + k] = ready.astype(BF16)
            at = slice(k * BLOCK, (k + 1) * BLOCK)
            state = half * (ready + dot(b_t[:, at], scaled[b][at, :]))
        for g in range(STATE // 8):
            sent[b, g, :, :inner] = state[8 * g : 8 * g + 8].astype(BF16)
            sent[b, g, :, inner:] = decays[b][...]


def scan_kernel(got, out, table, logs):
    devices, _, width = got.shape
    inner = width - LANES
    for s in range(devices):
        parts = got[s, :, inner:].astype(F32)
        table[s : s + 1, :] = parts[0:1] + parts[1:2] + parts[2:3]
    logs[...] = jnp.exp(over_channels(table[...], head_lanes(inner)))
    state = jnp.zeros((8, inner), F32)
    for s in range(devices):
        out[s] = state.astype(BF16)
        state = logs[s : s + 1, :] * state + got[s, :, :inner].astype(F32)


def gated_kernel(batch, length, arrived, b_rows, c_rows, starts, *refs):
    scaled, refs = refs[:batch], refs[batch:]
    opened, refs = refs[:batch], refs[batch:]
    rows, (gated, squares) = refs[:batch], refs[batch:]
    blocks = length // BLOCK
    ones = jnp.ones((8, gated.shape[1]), BF16)
    i = lax.broadcasted_iota(jnp.int32, (BLOCK, BLOCK), 0)
    j = lax.broadcasted_iota(jnp.int32, (BLOCK, BLOCK), 1)
    for b in range(batch):
        for k in range(blocks):
            n = b * blocks + k
            at = slice(k * BLOCK, (k + 1) * BLOCK)
            c = c_rows[n * BLOCK : (n + 1) * BLOCK, :]
            scores = dot(c, b_rows[b, :, at])
            scores = jnp.where(i >= j, scores, 0.0).astype(BF16)
            y = dot(scores, scaled[b][at, :]) + dot(c, starts[n])
            y = y + rows[b][blocks + k : blocks + k + 1, :] * dot(c, arrived[b])
            g = y * opened[b][at, :].astype(F32)
            gated[n * BLOCK : (n + 1) * BLOCK, :] = g
            squares[:, n, :] = dot_nt(ones, (g * g).astype(BF16))


def scale_kernel(gated, squares, gain, out):
    total = squares[0]
    for d in range(1, squares.shape[0]):
        total = total + squares[d]
    scale = lax.rsqrt(total / DI + EPSILON)
    count = scale.shape[0]
    scale = jnp.concatenate([scale, jnp.zeros((LANES - count, LANES), F32)], axis=0)
    columns = jnp.transpose(scale)
    for n in range(count):
        at = slice(n * LANES, (n + 1) * LANES)
        out[at, :] = (gated[at, :] * columns[:, n : n + 1] * gain[...][None, :]).astype(BF16)


ANY = pl.BlockSpec(memory_space=pl.ANY)
WHOLE = pl.BlockSpec(memory_space=pltpu.VMEM)


def call(kernel, out, ins=None, scratch=(), mib=12, flops=0, outs=None, grid=()):
    shapes = [jax.ShapeDtypeStruct(s, d) for s, d in out]
    specs = {} if ins is None else {"in_specs": ins}
    if outs is not None:
        specs["out_specs"] = outs if len(outs) > 1 else outs[0]
    return pl.pallas_call(
        kernel,
        out_shape=shapes if len(shapes) > 1 else shapes[0],
        grid=grid,
        scratch_shapes=[s if not isinstance(s, tuple) else pltpu.VMEM(*s) for s in scratch],
        compiler_params=pltpu.CompilerParams(vmem_limit_bytes=mib << 20),
        cost_estimate=pl.CostEstimate(flops=flops, transcendentals=0, bytes_accessed=0)
        if flops
        else None,
        **specs,
    )


def on_device(
    hidden_in, gate_proj, value_proj, bc_proj, step_proj, value_conv, bc_conv, step_bias, log_rate,
    norm_gain,
):
    batch, length, width = hidden_in.shape
    tokens = batch * length
    inner = value_proj.shape[1]
    heads = step_proj.shape[1]
    share = bc_proj.shape[1]
    states = 2 * STATE
    blocks = tokens // BLOCK
    seq, tp = lax.axis_size("seq"), lax.axis_size("tp")
    hidden = hidden_in.reshape(tokens, width)
    weight = bc_proj.T
    step_weight = step_proj.T
    place = lax.axis_index("tp").reshape(1)
    smem = pl.BlockSpec(memory_space=pltpu.SMEM)
    tail = hidden_in[:, length - 8 :, :]
    halo = lax.ppermute(tail, "seq", [(i, i + 1) for i in range(seq - 1)]).reshape(8 * batch, width)
    own = call(
        functools.partial(bc_kernel, 256),
        [((share, tokens), BF16)],
        scratch=[((256, LANES), F32)],
        flops=2 * tokens * width * share,
    )(hidden, weight)
    shard = call(
        functools.partial(join_kernel, batch),
        [((share, tokens + LANES), BF16)],
        scratch=[((LANES, LANES), F32)],
    )(halo, weight, own)
    work = 2 * length * width * inner

    def value_of(b, hidden):
        return call(
            functools.partial(value_kernel, b, length),
            [
                ((length, inner), BF16),
                ((length, LANES), F32),
                ((2 * length // BLOCK, inner), F32),
                ((8, LANES), BF16),
            ],
            ins=[smem] * 2 + [WHOLE] * 5,
            outs=[WHOLE] * 4,
            scratch=[((length + 8, inner), F32), ((LANES, width), BF16)],
            flops=work,
        )(step_bias, log_rate, hidden, halo, value_proj, value_conv, step_weight)

    def gate_of(b, hidden, opening):
        return call(
            functools.partial(gate_kernel, b, length), [((length, inner), BF16)], flops=work
        )(hidden, gate_proj, opening)

    up = [(i, (i + 1) % tp) for i in range(tp)]
    down = [(i, (i - 1) % tp) for i in range(tp)]
    shards, places = [shard], [0]
    left = right = shard
    scaled, openings, rows, decays, opened = [], [], [], [], []
    for r in range(tp // 2):
        to_left = lax.ppermute(right, "tp", down) if 2 * r + 2 < tp else right
        to_right = lax.ppermute(left, "tp", up)
        if r < batch:
            one = value_of(r, hidden)
            for where, part in zip((scaled, openings, rows, decays), one):
                where.append(part)
            mark = one[3]
        elif r < 2 * batch:
            mark = gate_of(r - batch, hidden, openings[r - batch])
            opened.append(mark)
        left, right, hidden, mark = lax.optimization_barrier((to_right, to_left, hidden, mark))
        if r < batch:
            decays[-1] = mark
        else:
            opened[-1] = mark
        shards.append(left)
        places.append(tp - r - 1)
        if 2 * r + 2 < tp:
            shards.append(right)
            places.append(r + 1)
    b_rows, c_rows, starts, sent = call(
        functools.partial(state_kernel, batch, length, places),
        [
            ((batch, STATE, length), BF16),
            ((tokens, STATE), BF16),
            ((blocks, STATE, inner), BF16),
            ((batch, STATE // 8, 8, inner + LANES), BF16),
        ],
        ins=[smem] + [WHOLE] * (1 + tp + 3 * batch),
        outs=[WHOLE] * 4,
        scratch=[((states, tokens), F32), ((states, LANES), F32)],
    )(place, bc_conv, *shards, *scaled, *rows, *decays)
    got = lax.all_to_all(sent.reshape(seq, -1, inner + LANES), "seq", 0, 0, tiled=True)
    prefix = call(
        scan_kernel,
        [((seq, 8, inner), BF16)],
        scratch=[((seq, LANES), F32), ((seq, inner), F32)],
    )(got)
    arrived = lax.all_to_all(prefix, "seq", 0, 0, tiled=True).reshape(batch, STATE, inner)
    gated, squares = call(
        functools.partial(gated_kernel, batch, length),
        [((tokens, inner), F32), ((tp, blocks, LANES), F32)],
    )(arrived, b_rows, c_rows, starts, *scaled, *opened, *rows)
    whole = lax.all_to_all(squares, "tp", 0, 0, tiled=True)
    out = call(scale_kernel, [((tokens, inner), BF16)])(gated, whole, norm_gain)
    return out.reshape(batch, length, inner)


def solution(mesh):
    placed = (
        P(None, "seq", None),
        P(None, "tp"),
        P(None, "tp"),
        P(None, "tp"),
        P(None, "tp"),
        P(None, "tp"),
        P(),
        P("tp"),
        P("tp"),
        P("tp"),
    )
    return jax.shard_map(
        on_device, mesh=mesh, in_specs=placed, out_specs=P(None, "seq", "tp"), check_vma=False
    )
```

```python
import functools

import jax
import jax.numpy as jnp
from jax import lax
from jax.experimental import pallas as pl
from jax.experimental.pallas import tpu as pltpu
from jax.sharding import Mesh
from jax.sharding import PartitionSpec as P

DI = 5120
HEAD_DIM = 64
STATE = 128
CONV = 4
BLOCK = 128
LANES = 128
EPSILON = 1e-05

F32 = jnp.float32
BF16 = jnp.bfloat16
HIGHEST = lax.Precision.HIGHEST
NT = (((1,), (1,)), ((), ()))


def dot(a, b):
    return jnp.dot(a, b, preferred_element_type=F32)


def dot_nt(a, b):
    return lax.dot_general(a, b, NT, preferred_element_type=F32)


def silu(x):
    half = 0.5 * x
    return half + half * jnp.tanh(half)


def split_in_three(x):
    high = x.astype(BF16)
    rest = x - high.astype(F32)
    middle = rest.astype(BF16)
    return high, middle, (rest - middle.astype(F32)).astype(BF16)


def head_lanes(width):
    head = lax.broadcasted_iota(jnp.int32, (2 * LANES, width), 1) // HEAD_DIM
    row = lax.broadcasted_iota(jnp.int32, (2 * LANES, width), 0)
    return (head == lax.rem(row, LANES)).astype(BF16)


def over_channels(x, spread):
    high, middle, _ = split_in_three(x)
    return dot(jnp.concatenate([high, middle], axis=1), spread)


def transposed(part, pad):
    pad[:, : part.shape[1]] = part
    return jnp.transpose(pad[...])[: part.shape[1]].astype(BF16)


def bc_kernel(chunk, hidden, weight, out, pad):
    pad[...] = jnp.zeros_like(pad)
    for r in range(0, hidden.shape[0], chunk):
        part = dot_nt(hidden[r : r + chunk, :], weight[...])
        out[:, r : r + chunk] = transposed(part, pad)


def join_kernel(batch, halo, weight, own, out, pad):
    share = weight.shape[0]
    before = dot_nt(halo[...], weight[...])
    pad[...] = jnp.zeros_like(pad)
    for b in range(batch):
        pad[LANES - 8 - 64 * b : LANES - 64 * b, :share] = before[8 * b : 8 * b + 8]
    out[:, :LANES] = jnp.transpose(pad[...])[:share].astype(BF16)
    out[:, LANES:] = own[...]


def value_kernel(
    b, length, step_bias, log_rate, hidden, halo, weight, taps, step_weight,
    scaled, opening, rows, decays, padded, step_pad,
):
    inner = weight.shape[1]
    heads = step_weight.shape[0]
    spread = head_lanes(inner)
    step_pad[...] = jnp.zeros_like(step_pad)
    step_pad[:heads, :] = step_weight[...]
    lane = lax.broadcasted_iota(jnp.int32, (1, LANES), 1)
    bias, rate = jnp.zeros((1, LANES), F32), jnp.full((1, LANES), -1e30, F32)
    for h in range(heads):
        bias = jnp.where(lane == h, step_bias[h], bias)
        rate = jnp.where(lane == h, log_rate[h], rate)
    rate = jnp.exp(rate)
    own = hidden[b * length : (b + 1) * length, :]
    before = dot(halo[...], weight[...]).astype(BF16).astype(F32)
    padded[0:8, :] = before[8 * b : 8 * b + 8]
    padded[8 : 8 + length, :] = dot(own, weight[...]).astype(BF16).astype(F32)
    step_pre = dot_nt(own, step_pad[...]) + bias
    steps = jnp.maximum(step_pre, 0.0) + jnp.log1p(jnp.exp(-jnp.abs(step_pre)))
    width = 3 * BLOCK
    i = lax.broadcasted_iota(jnp.int32, (BLOCK, width), 0)
    j = lax.rem(lax.broadcasted_iota(jnp.int32, (BLOCK, width), 1), BLOCK)
    lower = (i >= j).astype(BF16)
    blocks = range(0, length, BLOCK)
    parts = split_in_three(-steps * rate)
    side = [jnp.concatenate([part[r : r + BLOCK] for r in blocks], axis=1) for part in parts]
    cumulative = dot(lower, jnp.concatenate(side, axis=0))
    half = 0.5 * cumulative[BLOCK - 1 : BLOCK, :]
    centered = cumulative - half
    ahead = jnp.exp(-centered)
    behind = jnp.exp(centered)
    ahead = jnp.concatenate([ahead[:, k * LANES : (k + 1) * LANES] for k in range(len(blocks))], axis=0)
    ahead = over_channels(ahead * steps, spread)
    total = jnp.zeros((1, LANES), F32)
    halves, offsets = [], []
    for k, r in enumerate(blocks):
        lanes = slice(k * LANES, (k + 1) * LANES)
        halves.append(half[:, lanes])
        offsets.append(total + half[:, lanes])
        total = total + 2.0 * half[:, lanes]
        value = sum(taps[t : t + 1, :] * padded[r + 5 + t : r + 5 + t + BLOCK, :] for t in range(CONV))
        scaled[r : r + BLOCK, :] = (silu(value) * ahead[r : r + BLOCK]).astype(BF16)
        opening[r : r + BLOCK, :] = behind[:, lanes]
    high, middle, low = split_in_three(total)
    decays[...] = jnp.concatenate([high, middle, low, jnp.zeros((5, LANES), BF16)], axis=0)
    rows[...] = jnp.exp(over_channels(jnp.concatenate(halves + offsets, axis=0), spread))


def gate_kernel(b, length, hidden, weight, opening, out):
    gate = dot(hidden[b * length : (b + 1) * length, :], weight[...]).astype(BF16).astype(F32)
    out[...] = (silu(gate) * over_channels(opening[...], head_lanes(weight.shape[1]))).astype(BF16)


def state_kernel(batch, length, steps, place, taps, *refs):
    shards, refs = refs[: len(steps)], refs[len(steps) :]
    scaled, refs = refs[:batch], refs[batch:]
    rows, refs = refs[:batch], refs[batch:]
    decays, (b_rows, c_rows, starts, sent, mixed, columns) = refs[:batch], refs[batch:]
    blocks = length // BLOCK
    inner = scaled[0].shape[1]
    share = shards[0].shape[0]
    rest = jnp.zeros((LANES - CONV, 2 * STATE), F32)
    columns[...] = jnp.transpose(jnp.concatenate([taps[...], rest], axis=0))
    for step, shard in zip(steps, shards):
        first = pl.multiple_of(lax.rem(place[0] + step, len(steps)) * share, share)
        tap = columns[pl.ds(first, share), :]
        halo = shard[:, :LANES].astype(F32)
        for b in range(batch):
            own = shard[:, LANES + b * length : LANES + (b + 1) * length].astype(F32)
            before = pltpu.roll(halo, 64 * b, 1) if b else halo
            padded = jnp.concatenate([before, own], axis=1)
            total = tap[:, CONV - 1 : CONV] * own
            for t in range(CONV - 1):
                total = total + tap[:, t : t + 1] * pltpu.roll(padded, CONV - 1 - t, 1)[:, LANES:]
            mixed[pl.ds(first, share), b * length : (b + 1) * length] = silu(total)
    for b in range(batch):
        own = slice(b * length, (b + 1) * length)
        b_t = mixed[:STATE, own].astype(BF16)
        b_rows[b] = b_t
        c_rows[own, :] = jnp.transpose(mixed[STATE:, own]).astype(BF16)
        state = jnp.zeros((STATE, inner), F32)
        for k in range(blocks):
            half = rows[b][k : k + 1, :]
            ready = half * state
            starts[b * blocks + k] = ready.astype(BF16)
            at = slice(k * BLOCK, (k + 1) * BLOCK)
            state = half * (ready + dot(b_t[:, at], scaled[b][at, :]))
        for g in range(STATE // 8):
            sent[b, g, :, :inner] = state[8 * g : 8 * g + 8].astype(BF16)
            sent[b, g, :, inner:] = decays[b][...]


def scan_kernel(got, out, table, logs):
    devices, _, width = got.shape
    inner = width - LANES
    for s in range(devices):
        parts = got[s, :, inner:].astype(F32)
        table[s : s + 1, :] = parts[0:1] + parts[1:2] + parts[2:3]
    logs[...] = jnp.exp(over_channels(table[...], head_lanes(inner)))
    state = jnp.zeros((8, inner), F32)
    for s in range(devices):
        out[s] = state.astype(BF16)
        state = logs[s : s + 1, :] * state + got[s, :, :inner].astype(F32)


def gated_kernel(batch, length, arrived, b_rows, c_rows, starts, *refs):
    scaled, refs = refs[:batch], refs[batch:]
    opened, refs = refs[:batch], refs[batch:]
    rows, (gated, squares) = refs[:batch], refs[batch:]
    blocks = length // BLOCK
    ones = jnp.ones((8, gated.shape[1]), BF16)
    i = lax.broadcasted_iota(jnp.int32, (BLOCK, BLOCK), 0)
    j = lax.broadcasted_iota(jnp.int32, (BLOCK, BLOCK), 1)
    for b in range(batch):
        for k in range(blocks):
            n = b * blocks + k
            at = slice(k * BLOCK, (k + 1) * BLOCK)
            c = c_rows[n * BLOCK : (n + 1) * BLOCK, :]
            scores = dot(c, b_rows[b, :, at])
            scores = jnp.where(i >= j, scores, 0.0).astype(BF16)
            y = dot(scores, scaled[b][at, :]) + dot(c, starts[n])
            y = y + rows[b][blocks + k : blocks + k + 1, :] * dot(c, arrived[b])
            g = y * opened[b][at, :].astype(F32)
            gated[n * BLOCK : (n + 1) * BLOCK, :] = g
            squares[:, n, :] = dot_nt(ones, (g * g).astype(BF16))


def scale_kernel(gated, squares, gain, out):
    total = squares[0]
    for d in range(1, squares.shape[0]):
        total = total + squares[d]
    scale = lax.rsqrt(total / DI + EPSILON)
    count = scale.shape[0]
    scale = jnp.concatenate([scale, jnp.zeros((LANES - count, LANES), F32)], axis=0)
    columns = jnp.transpose(scale)
    for n in range(count):
        at = slice(n * LANES, (n + 1) * LANES)
        out[at, :] = (gated[at, :] * columns[:, n : n + 1] * gain[...][None, :]).astype(BF16)


ANY = pl.BlockSpec(memory_space=pl.ANY)
WHOLE = pl.BlockSpec(memory_space=pltpu.VMEM)


def call(kernel, out, ins=None, scratch=(), mib=12, flops=0, outs=None, grid=()):
    shapes = [jax.ShapeDtypeStruct(s, d) for s, d in out]
    specs = {} if ins is None else {"in_specs": ins}
    if outs is not None:
        specs["out_specs"] = outs if len(outs) > 1 else outs[0]
    return pl.pallas_call(
        kernel,
        out_shape=shapes if len(shapes) > 1 else shapes[0],
        grid=grid,
        scratch_shapes=[s if not isinstance(s, tuple) else pltpu.VMEM(*s) for s in scratch],
        compiler_params=pltpu.CompilerParams(vmem_limit_bytes=mib << 20),
        cost_estimate=pl.CostEstimate(flops=flops, transcendentals=0, bytes_accessed=0)
        if flops
        else None,
        **specs,
    )


def on_device(
    hidden_in, gate_proj, value_proj, bc_proj, step_proj, value_conv, bc_conv, step_bias, log_rate,
    norm_gain,
):
    batch, length, width = hidden_in.shape
    tokens = batch * length
    inner = value_proj.shape[1]
    heads = step_proj.shape[1]
    share = bc_proj.shape[1]
    states = 2 * STATE
    blocks = tokens // BLOCK
    seq, tp = lax.axis_size("seq"), lax.axis_size("tp")
    hidden = hidden_in.reshape(tokens, width)
    weight = bc_proj.T
    step_weight = step_proj.T
    place = lax.axis_index("tp").reshape(1)
    smem = pl.BlockSpec(memory_space=pltpu.SMEM)
    tail = hidden_in[:, length - 8 :, :]
    halo = lax.ppermute(tail, "seq", [(i, i + 1) for i in range(seq - 1)]).reshape(8 * batch, width)
    own = call(
        functools.partial(bc_kernel, 256),
        [((share, tokens), BF16)],
        scratch=[((256, LANES), F32)],
        flops=6 * tokens * width * share,
    )(hidden, weight)
    shard = call(
        functools.partial(join_kernel, batch),
        [((share, tokens + LANES), BF16)],
        scratch=[((LANES, LANES), F32)],
        flops=30 * tokens * width * share,
    )(halo, weight, own)
    work = 2 * length * width * inner

    def value_of(b, hidden):
        return call(
            functools.partial(value_kernel, b, length),
            [
                ((length, inner), BF16),
                ((length, LANES), F32),
                ((2 * length // BLOCK, inner), F32),
                ((8, LANES), BF16),
            ],
            ins=[smem] * 2 + [WHOLE] * 5,
            outs=[WHOLE] * 4,
            scratch=[((length + 8, inner), F32), ((LANES, width), BF16)],
            flops=work,
        )(step_bias, log_rate, hidden, halo, value_proj, value_conv, step_weight)

    def gate_of(b, hidden, opening):
        return call(
            functools.partial(gate_kernel, b, length), [((length, inner), BF16)], flops=work
        )(hidden, gate_proj, opening)

    up = [(i, (i + 1) % tp) for i in range(tp)]
    down = [(i, (i - 1) % tp) for i in range(tp)]
    shards, places = [shard], [0]
    left = right = shard
    scaled, openings, rows, decays, opened = [], [], [], [], []
    for r in range(tp // 2):
        to_left = lax.ppermute(right, "tp", down) if 2 * r + 2 < tp else right
        to_right = lax.ppermute(left, "tp", up)
        if r < batch:
            one = value_of(r, hidden)
            for where, part in zip((scaled, openings, rows, decays), one):
                where.append(part)
            mark = one[3]
        elif r < 2 * batch:
            mark = gate_of(r - batch, hidden, openings[r - batch])
            opened.append(mark)
        left, right, hidden, mark = lax.optimization_barrier((to_right, to_left, hidden, mark))
        if r < batch:
            decays[-1] = mark
        else:
            opened[-1] = mark
        shards.append(left)
        places.append(tp - r - 1)
        if 2 * r + 2 < tp:
            shards.append(right)
            places.append(r + 1)
    b_rows, c_rows, starts, sent = call(
        functools.partial(state_kernel, batch, length, places),
        [
            ((batch, STATE, length), BF16),
            ((tokens, STATE), BF16),
            ((blocks, STATE, inner), BF16),
            ((batch, STATE // 8, 8, inner + LANES), BF16),
        ],
        ins=[smem] + [WHOLE] * (1 + tp + 3 * batch),
        outs=[WHOLE] * 4,
        scratch=[((states, tokens), F32), ((states, LANES), F32)],
    )(place, bc_conv, *shards, *scaled, *rows, *decays)
    got = lax.all_to_all(sent.reshape(seq, -1, inner + LANES), "seq", 0, 0, tiled=True)
    prefix = call(
        scan_kernel,
        [((seq, 8, inner), BF16)],
        scratch=[((seq, LANES), F32), ((seq, inner), F32)],
    )(got)
    arrived = lax.all_to_all(prefix, "seq", 0, 0, tiled=True).reshape(batch, STATE, inner)
    gated, squares = call(
        functools.partial(gated_kernel, batch, length),
        [((tokens, inner), F32), ((tp, blocks, LANES), F32)],
    )(arrived, b_rows, c_rows, starts, *scaled, *opened, *rows)
    whole = lax.all_to_all(squares, "tp", 0, 0, tiled=True)
    out = call(scale_kernel, [((tokens, inner), BF16)])(gated, whole, norm_gain)
    return out.reshape(batch, length, inner)


def solution(mesh):
    placed = (
        P(None, "seq", None),
        P(None, "tp"),
        P(None, "tp"),
        P(None, "tp"),
        P(None, "tp"),
        P(None, "tp"),
        P(),
        P("tp"),
        P("tp"),
        P("tp"),
    )
    return jax.shard_map(
        on_device, mesh=mesh, in_specs=placed, out_specs=P(None, "seq", "tp"), check_vma=False
    )
```

```python
import functools

import jax
import jax.numpy as jnp
from jax import lax
from jax.experimental import pallas as pl
from jax.experimental.pallas import tpu as pltpu
from jax.sharding import Mesh
from jax.sharding import PartitionSpec as P

DI = 5120
HEAD_DIM = 64
STATE = 128
CONV = 4
BLOCK = 128
LANES = 128
EPSILON = 1e-05

F32 = jnp.float32
BF16 = jnp.bfloat16
HIGHEST = lax.Precision.HIGHEST
NT = (((1,), (1,)), ((), ()))


def dot(a, b):
    return jnp.dot(a, b, preferred_element_type=F32)


def dot_nt(a, b):
    return lax.dot_general(a, b, NT, preferred_element_type=F32)


def silu(x):
    half = 0.5 * x
    return half + half * jnp.tanh(half)


def split_in_three(x):
    high = x.astype(BF16)
    rest = x - high.astype(F32)
    middle = rest.astype(BF16)
    return high, middle, (rest - middle.astype(F32)).astype(BF16)


def head_lanes(width):
    head = lax.broadcasted_iota(jnp.int32, (2 * LANES, width), 1) // HEAD_DIM
    row = lax.broadcasted_iota(jnp.int32, (2 * LANES, width), 0)
    return (head == lax.rem(row, LANES)).astype(BF16)


def over_channels(x, spread):
    high, middle, _ = split_in_three(x)
    return dot(jnp.concatenate([high, middle], axis=1), spread)


def bc_kernel(chunk, hidden, weight, step_weight, out, steps, pad, joined):
    share = weight.shape[0]
    joined[...] = jnp.zeros_like(joined)
    joined[: step_weight.shape[0], :] = step_weight[...]
    joined[16 : 16 + share, :] = weight[...]
    pad[...] = jnp.zeros_like(pad)
    for r in range(0, hidden.shape[0], chunk):
        pad[:, : 16 + share] = dot_nt(hidden[r : r + chunk, :], joined[...])
        steps[r : r + chunk, :] = pad[...]
        out[:, r : r + chunk] = jnp.transpose(pad[...])[16 : 16 + share].astype(BF16)


def join_kernel(batch, halo, weight, own, out, pad):
    share = weight.shape[0]
    before = dot_nt(halo[...], weight[...])
    pad[...] = jnp.zeros_like(pad)
    for b in range(batch):
        pad[LANES - 8 - 64 * b : LANES - 64 * b, :share] = before[8 * b : 8 * b + 8]
    out[:, :LANES] = jnp.transpose(pad[...])[:share].astype(BF16)
    out[:, LANES:] = own[...]


def value_kernel(
    b, length, heads, step_bias, log_rate, hidden, halo, weight, taps, steps_in,
    scaled, opening, rows, decays, padded,
):
    inner = weight.shape[1]
    spread = head_lanes(inner)
    lane = lax.broadcasted_iota(jnp.int32, (1, LANES), 1)
    bias, rate = jnp.zeros((1, LANES), F32), jnp.full((1, LANES), -1e30, F32)
    for h in range(heads):
        bias = jnp.where(lane == h, step_bias[h], bias)
        rate = jnp.where(lane == h, log_rate[h], rate)
    rate = jnp.exp(rate)
    own = slice(b * length, (b + 1) * length)
    both = jnp.concatenate([halo[...], hidden[own, :]], axis=0)
    first = halo.shape[0]
    both = dot(both, weight[...]).astype(BF16).astype(F32)
    padded[0:8, :] = both[8 * b : 8 * b + 8]
    padded[8:, :] = both[first:]
    step_pre = steps_in[own, :] + bias
    steps = jnp.maximum(step_pre, 0.0) + jnp.log1p(jnp.exp(-jnp.abs(step_pre)))
    width = 3 * BLOCK
    i = lax.broadcasted_iota(jnp.int32, (BLOCK, width), 0)
    j = lax.rem(lax.broadcasted_iota(jnp.int32, (BLOCK, width), 1), BLOCK)
    lower = (i >= j).astype(BF16)
    blocks = range(0, length, BLOCK)
    parts = split_in_three(-steps * rate)
    side = [jnp.concatenate([part[r : r + BLOCK] for r in blocks], axis=1) for part in parts]
    cumulative = dot(lower, jnp.concatenate(side, axis=0))
    half = 0.5 * cumulative[BLOCK - 1 : BLOCK, :]
    centered = cumulative - half
    ahead = jnp.exp(-centered)
    behind = jnp.exp(centered)
    ahead = jnp.concatenate([ahead[:, k * LANES : (k + 1) * LANES] for k in range(len(blocks))], axis=0)
    ahead = over_channels(ahead * steps, spread)
    total = jnp.zeros((1, LANES), F32)
    halves, offsets = [], []
    for k, r in enumerate(blocks):
        lanes = slice(k * LANES, (k + 1) * LANES)
        halves.append(half[:, lanes])
        offsets.append(total + half[:, lanes])
        total = total + 2.0 * half[:, lanes]
        value = sum(taps[t : t + 1, :] * padded[r + 5 + t : r + 5 + t + BLOCK, :] for t in range(CONV))
        scaled[r : r + BLOCK, :] = (silu(value) * ahead[r : r + BLOCK]).astype(BF16)
        opening[r : r + BLOCK, :] = behind[:, lanes]
    high, middle, low = split_in_three(total)
    decays[...] = jnp.concatenate([high, middle, low, jnp.zeros((5, LANES), BF16)], axis=0)
    rows[...] = jnp.exp(over_channels(jnp.concatenate(halves + offsets, axis=0), spread))


def gate_kernel(b, length, hidden, weight, opening, out):
    gate = dot(hidden[b * length : (b + 1) * length, :], weight[...]).astype(BF16).astype(F32)
    out[...] = (silu(gate) * over_channels(opening[...], head_lanes(weight.shape[1]))).astype(BF16)


def state_kernel(batch, length, steps, place, taps, *refs):
    shards, refs = refs[: len(steps)], refs[len(steps) :]
    scaled, refs = refs[:batch], refs[batch:]
    rows, refs = refs[:batch], refs[batch:]
    decays, (b_rows, c_rows, starts, sent, mixed, columns) = refs[:batch], refs[batch:]
    blocks = length // BLOCK
    inner = scaled[0].shape[1]
    share = shards[0].shape[0]
    rest = jnp.zeros((LANES - CONV, 2 * STATE), F32)
    columns[...] = jnp.transpose(jnp.concatenate([taps[...], rest], axis=0))
    for step, shard in zip(steps, shards):
        first = pl.multiple_of(lax.rem(place[0] + step, len(steps)) * share, share)
        tap = columns[pl.ds(first, share), :]
        halo = shard[:, :LANES].astype(F32)
        for b in range(batch):
            own = shard[:, LANES + b * length : LANES + (b + 1) * length].astype(F32)
            before = pltpu.roll(halo, 64 * b, 1) if b else halo
            padded = jnp.concatenate([before, own], axis=1)
            total = tap[:, CONV - 1 : CONV] * own
            for t in range(CONV - 1):
                total = total + tap[:, t : t + 1] * pltpu.roll(padded, CONV - 1 - t, 1)[:, LANES:]
            mixed[pl.ds(first, share), b * length : (b + 1) * length] = silu(total)
    for b in range(batch):
        own = slice(b * length, (b + 1) * length)
        b_t = mixed[:STATE, own].astype(BF16)
        b_rows[b] = b_t
        c_rows[own, :] = jnp.transpose(mixed[STATE:, own]).astype(BF16)
        state = jnp.zeros((STATE, inner), F32)
        for k in range(blocks):
            half = rows[b][k : k + 1, :]
            ready = half * state
            starts[b * blocks + k] = ready.astype(BF16)
            at = slice(k * BLOCK, (k + 1) * BLOCK)
            state = half * (ready + dot(b_t[:, at], scaled[b][at, :]))
        for g in range(STATE // 8):
            sent[b, g, :, :inner] = state[8 * g : 8 * g + 8].astype(BF16)
            sent[b, g, :, inner:] = decays[b][...]


def scan_kernel(got, out, table, logs):
    devices, _, width = got.shape
    inner = width - LANES
    for s in range(devices):
        parts = got[s, :, inner:].astype(F32)
        table[s : s + 1, :] = parts[0:1] + parts[1:2] + parts[2:3]
    logs[...] = jnp.exp(over_channels(table[...], head_lanes(inner)))
    state = jnp.zeros((8, inner), F32)
    for s in range(devices):
        out[s] = state.astype(BF16)
        state = logs[s : s + 1, :] * state + got[s, :, :inner].astype(F32)


def gated_kernel(batch, length, arrived, b_rows, c_rows, starts, *refs):
    scaled, refs = refs[:batch], refs[batch:]
    opened, refs = refs[:batch], refs[batch:]
    rows, (gated, squares) = refs[:batch], refs[batch:]
    blocks = length // BLOCK
    ones = jnp.ones((8, gated.shape[1]), BF16)
    i = lax.broadcasted_iota(jnp.int32, (BLOCK, BLOCK), 0)
    j = lax.broadcasted_iota(jnp.int32, (BLOCK, BLOCK), 1)
    for b in range(batch):
        for k in range(blocks):
            n = b * blocks + k
            at = slice(k * BLOCK, (k + 1) * BLOCK)
            c = c_rows[n * BLOCK : (n + 1) * BLOCK, :]
            scores = dot(c, b_rows[b, :, at])
            scores = jnp.where(i >= j, scores, 0.0).astype(BF16)
            y = dot(scores, scaled[b][at, :]) + dot(c, starts[n])
            y = y + rows[b][blocks + k : blocks + k + 1, :] * dot(c, arrived[b])
            g = y * opened[b][at, :].astype(F32)
            gated[n * BLOCK : (n + 1) * BLOCK, :] = g
            squares[:, n, :] = dot_nt(ones, (g * g).astype(BF16))


def scale_kernel(gated, squares, gain, out):
    total = squares[0]
    for d in range(1, squares.shape[0]):
        total = total + squares[d]
    scale = lax.rsqrt(total / DI + EPSILON)
    count = scale.shape[0]
    scale = jnp.concatenate([scale, jnp.zeros((LANES - count, LANES), F32)], axis=0)
    columns = jnp.transpose(scale)
    for n in range(count):
        at = slice(n * LANES, (n + 1) * LANES)
        out[at, :] = (gated[at, :] * columns[:, n : n + 1] * gain[...][None, :]).astype(BF16)


ANY = pl.BlockSpec(memory_space=pl.ANY)
WHOLE = pl.BlockSpec(memory_space=pltpu.VMEM)


def call(kernel, out, ins=None, scratch=(), mib=12, flops=0, outs=None, grid=()):
    shapes = [jax.ShapeDtypeStruct(s, d) for s, d in out]
    specs = {} if ins is None else {"in_specs": ins}
    if outs is not None:
        specs["out_specs"] = outs if len(outs) > 1 else outs[0]
    return pl.pallas_call(
        kernel,
        out_shape=shapes if len(shapes) > 1 else shapes[0],
        grid=grid,
        scratch_shapes=[s if not isinstance(s, tuple) else pltpu.VMEM(*s) for s in scratch],
        compiler_params=pltpu.CompilerParams(vmem_limit_bytes=mib << 20),
        cost_estimate=pl.CostEstimate(flops=flops, transcendentals=0, bytes_accessed=0)
        if flops
        else None,
        **specs,
    )


def on_device(
    hidden_in, gate_proj, value_proj, bc_proj, step_proj, value_conv, bc_conv, step_bias, log_rate,
    norm_gain,
):
    batch, length, width = hidden_in.shape
    tokens = batch * length
    inner = value_proj.shape[1]
    heads = step_proj.shape[1]
    share = bc_proj.shape[1]
    states = 2 * STATE
    blocks = tokens // BLOCK
    seq, tp = lax.axis_size("seq"), lax.axis_size("tp")
    hidden = hidden_in.reshape(tokens, width)
    weight = bc_proj.T
    step_weight = step_proj.T
    place = lax.axis_index("tp").reshape(1)
    smem = pl.BlockSpec(memory_space=pltpu.SMEM)
    tail = hidden_in[:, length - 8 :, :]
    halo = lax.ppermute(tail, "seq", [(i, i + 1) for i in range(seq - 1)]).reshape(8 * batch, width)
    own, step_pre = call(
        functools.partial(bc_kernel, 256),
        [((share, tokens), BF16), ((tokens, LANES), F32)],
        scratch=[((256, LANES), F32), ((16 + share, width), BF16)],
        flops=6 * tokens * width * share,
    )(hidden, weight, step_weight)
    shard = call(
        functools.partial(join_kernel, batch),
        [((share, tokens + LANES), BF16)],
        scratch=[((LANES, LANES), F32)],
        flops=30 * tokens * width * share,
    )(halo, weight, own)
    work = 2 * length * width * inner

    def value_of(b, hidden):
        return call(
            functools.partial(value_kernel, b, length, heads),
            [
                ((length, inner), BF16),
                ((length, LANES), F32),
                ((2 * length // BLOCK, inner), F32),
                ((8, LANES), BF16),
            ],
            ins=[smem] * 2 + [WHOLE] * 5,
            outs=[WHOLE] * 4,
            scratch=[((length + 8, inner), F32)],
            flops=work,
        )(step_bias, log_rate, hidden, halo, value_proj, value_conv, step_pre)

    def gate_of(b, hidden, opening):
        return call(
            functools.partial(gate_kernel, b, length), [((length, inner), BF16)], flops=work
        )(hidden, gate_proj, opening)

    up = [(i, (i + 1) % tp) for i in range(tp)]
    down = [(i, (i - 1) % tp) for i in range(tp)]
    shards, places = [shard], [0]
    left = right = shard
    scaled, openings, rows, decays, opened = [], [], [], [], []
    for r in range(tp // 2):
        to_left = lax.ppermute(right, "tp", down) if 2 * r + 2 < tp else right
        to_right = lax.ppermute(left, "tp", up)
        if r < batch:
            one = value_of(r, hidden)
            for where, part in zip((scaled, openings, rows, decays), one):
                where.append(part)
            mark = one[3]
        elif r < 2 * batch:
            mark = gate_of(r - batch, hidden, openings[r - batch])
            opened.append(mark)
        left, right, hidden, mark = lax.optimization_barrier((to_right, to_left, hidden, mark))
        if r < batch:
            decays[-1] = mark
        else:
            opened[-1] = mark
        shards.append(left)
        places.append(tp - r - 1)
        if 2 * r + 2 < tp:
            shards.append(right)
            places.append(r + 1)
    b_rows, c_rows, starts, sent = call(
        functools.partial(state_kernel, batch, length, places),
        [
            ((batch, STATE, length), BF16),
            ((tokens, STATE), BF16),
            ((blocks, STATE, inner), BF16),
            ((batch, STATE // 8, 8, inner + LANES), BF16),
        ],
        ins=[smem] + [WHOLE] * (1 + tp + 3 * batch),
        outs=[WHOLE] * 4,
        scratch=[((states, tokens), F32), ((states, LANES), F32)],
    )(place, bc_conv, *shards, *scaled, *rows, *decays)
    got = lax.all_to_all(sent.reshape(seq, -1, inner + LANES), "seq", 0, 0, tiled=True)
    prefix = call(
        scan_kernel,
        [((seq, 8, inner), BF16)],
        scratch=[((seq, LANES), F32), ((seq, inner), F32)],
    )(got)
    arrived = lax.all_to_all(prefix, "seq", 0, 0, tiled=True).reshape(batch, STATE, inner)
    gated, squares = call(
        functools.partial(gated_kernel, batch, length),
        [((tokens, inner), F32), ((tp, blocks, LANES), F32)],
    )(arrived, b_rows, c_rows, starts, *scaled, *opened, *rows)
    whole = lax.all_to_all(squares, "tp", 0, 0, tiled=True)
    out = call(scale_kernel, [((tokens, inner), BF16)])(gated, whole, norm_gain)
    return out.reshape(batch, length, inner)


def solution(mesh):
    placed = (
        P(None, "seq", None),
        P(None, "tp"),
        P(None, "tp"),
        P(None, "tp"),
        P(None, "tp"),
        P(None, "tp"),
        P(),
        P("tp"),
        P("tp"),
        P("tp"),
    )
    return jax.shard_map(
        on_device, mesh=mesh, in_specs=placed, out_specs=P(None, "seq", "tp"), check_vma=False
    )
```

```python
import functools

import jax
import jax.numpy as jnp
from jax import lax
from jax.experimental import pallas as pl
from jax.experimental.pallas import tpu as pltpu
from jax.sharding import Mesh
from jax.sharding import PartitionSpec as P

DI = 5120
HEAD_DIM = 64
STATE = 128
CONV = 4
BLOCK = 128
WAYS = 4
LANES = 128
EPSILON = 1e-05

F32 = jnp.float32
BF16 = jnp.bfloat16
HIGHEST = lax.Precision.HIGHEST
NT = (((1,), (1,)), ((), ()))


def dot(a, b):
    return jnp.dot(a, b, preferred_element_type=F32)


def dot_nt(a, b):
    return lax.dot_general(a, b, NT, preferred_element_type=F32)


def silu(x):
    half = 0.5 * x
    return half + half * jnp.tanh(half)


def split_in_three(x):
    high = x.astype(BF16)
    rest = x - high.astype(F32)
    middle = rest.astype(BF16)
    return high, middle, (rest - middle.astype(F32)).astype(BF16)


def head_lanes(width):
    head = lax.broadcasted_iota(jnp.int32, (2 * LANES, width), 1) // HEAD_DIM
    row = lax.broadcasted_iota(jnp.int32, (2 * LANES, width), 0)
    return (head == lax.rem(row, LANES)).astype(BF16)


def over_channels(x, spread):
    high, middle, _ = split_in_three(x)
    return dot(jnp.concatenate([high, middle], axis=1), spread)


def bc_kernel(chunk, hidden, weight, step_weight, out, steps, pad, joined):
    share = weight.shape[0]
    joined[...] = jnp.zeros_like(joined)
    joined[: step_weight.shape[0], :] = step_weight[...]
    joined[16 : 16 + share, :] = weight[...]
    pad[...] = jnp.zeros_like(pad)
    for r in range(0, hidden.shape[0], chunk):
        pad[:, : 16 + share] = dot_nt(hidden[r : r + chunk, :], joined[...])
        steps[r : r + chunk, :] = pad[...]
        out[:, r : r + chunk] = jnp.transpose(pad[...])[16 : 16 + share].astype(BF16)


def join_kernel(batch, halo, weight, own, out, pad):
    share = weight.shape[0]
    before = dot_nt(halo[...], weight[...])
    pad[...] = jnp.zeros_like(pad)
    for b in range(batch):
        pad[LANES - 8 - 64 * b : LANES - 64 * b, :share] = before[8 * b : 8 * b + 8]
    out[:, :LANES] = jnp.transpose(pad[...])[:share].astype(BF16)
    out[:, LANES:] = own[...]


def value_kernel(
    b, length, heads, step_bias, log_rate, hidden, halo, weight, taps, steps_in,
    scaled, opening, rows, decays, padded,
):
    inner = weight.shape[1]
    spread = head_lanes(inner)
    lane = lax.broadcasted_iota(jnp.int32, (1, LANES), 1)
    bias, rate = jnp.zeros((1, LANES), F32), jnp.full((1, LANES), -1e30, F32)
    for h in range(heads):
        bias = jnp.where(lane == h, step_bias[h], bias)
        rate = jnp.where(lane == h, log_rate[h], rate)
    rate = jnp.exp(rate)
    own = slice(b * length, (b + 1) * length)
    both = jnp.concatenate([halo[...], hidden[own, :]], axis=0)
    first = halo.shape[0]
    both = dot(both, weight[...]).astype(BF16).astype(F32)
    padded[0:8, :] = both[8 * b : 8 * b + 8]
    padded[8:, :] = both[first:]
    step_pre = steps_in[own, :] + bias
    steps = jnp.maximum(step_pre, 0.0) + jnp.log1p(jnp.exp(-jnp.abs(step_pre)))
    width = 3 * BLOCK
    i = lax.broadcasted_iota(jnp.int32, (BLOCK, width), 0)
    j = lax.rem(lax.broadcasted_iota(jnp.int32, (BLOCK, width), 1), BLOCK)
    lower = (i >= j).astype(BF16)
    blocks = range(0, length, BLOCK)
    parts = split_in_three(-steps * rate)
    side = [jnp.concatenate([part[r : r + BLOCK] for r in blocks], axis=1) for part in parts]
    cumulative = dot(lower, jnp.concatenate(side, axis=0))
    half = 0.5 * cumulative[BLOCK - 1 : BLOCK, :]
    centered = cumulative - half
    ahead = jnp.exp(-centered)
    behind = jnp.exp(centered)
    ahead = jnp.concatenate([ahead[:, k * LANES : (k + 1) * LANES] for k in range(len(blocks))], axis=0)
    ahead = over_channels(ahead * steps, spread)
    total = jnp.zeros((1, LANES), F32)
    halves, offsets = [], []
    for k, r in enumerate(blocks):
        lanes = slice(k * LANES, (k + 1) * LANES)
        halves.append(half[:, lanes])
        offsets.append(total + half[:, lanes])
        total = total + 2.0 * half[:, lanes]
        value = sum(taps[t : t + 1, :] * padded[r + 5 + t : r + 5 + t + BLOCK, :] for t in range(CONV))
        scaled[r : r + BLOCK, :] = (silu(value) * ahead[r : r + BLOCK]).astype(BF16)
        opening[r : r + BLOCK, :] = behind[:, lanes]
    high, middle, low = split_in_three(total)
    decays[...] = jnp.concatenate([high, middle, low, jnp.zeros((5, LANES), BF16)], axis=0)
    rows[...] = jnp.exp(over_channels(jnp.concatenate(halves + offsets, axis=0), spread))


def gate_kernel(b, length, hidden, weight, opening, out):
    gate = dot(hidden[b * length : (b + 1) * length, :], weight[...]).astype(BF16).astype(F32)
    out[...] = (silu(gate) * over_channels(opening[...], head_lanes(weight.shape[1]))).astype(BF16)


def state_kernel(batch, length, steps, place, taps, *refs):
    shards, refs = refs[: len(steps)], refs[len(steps) :]
    scaled, refs = refs[:batch], refs[batch:]
    rows, refs = refs[:batch], refs[batch:]
    decays, (b_rows, c_rows, starts, mine, other, mixed, columns) = refs[:batch], refs[batch:]
    blocks = length // BLOCK
    inner = scaled[0].shape[1]
    share = shards[0].shape[0]
    rest = jnp.zeros((LANES - CONV, 2 * STATE), F32)
    columns[...] = jnp.transpose(jnp.concatenate([taps[...], rest], axis=0))
    for step, shard in zip(steps, shards):
        first = pl.multiple_of(lax.rem(place[0] + step, len(steps)) * share, share)
        tap = columns[pl.ds(first, share), :]
        halo = shard[:, :LANES].astype(F32)
        for b in range(batch):
            own = shard[:, LANES + b * length : LANES + (b + 1) * length].astype(F32)
            before = pltpu.roll(halo, 64 * b, 1) if b else halo
            padded = jnp.concatenate([before, own], axis=1)
            total = tap[:, CONV - 1 : CONV] * own
            for t in range(CONV - 1):
                total = total + tap[:, t : t + 1] * pltpu.roll(padded, CONV - 1 - t, 1)[:, LANES:]
            mixed[pl.ds(first, share), b * length : (b + 1) * length] = silu(total)
    for b in range(batch):
        own = slice(b * length, (b + 1) * length)
        b_t = mixed[:STATE, own].astype(BF16)
        b_rows[b] = b_t
        c_rows[own, :] = jnp.transpose(mixed[STATE:, own]).astype(BF16)
        state = jnp.zeros((STATE, inner), F32)
        for k in range(blocks):
            half = rows[b][k : k + 1, :]
            ready = half * state
            starts[b * blocks + k] = ready.astype(BF16)
            at = slice(k * BLOCK, (k + 1) * BLOCK)
            state = half * (ready + dot(b_t[:, at], scaled[b][at, :]))

        def keep(target, state=state, b=b):
            for g in range(STATE // 8):
                target[g, :, :inner] = state[8 * g : 8 * g + 8].astype(BF16)
                target[g, :, inner:] = decays[b][...]

        pl.when(place[1] == b)(functools.partial(keep, mine))
        pl.when(place[1] != b)(functools.partial(keep, other))


def log_decay(state):
    parts = state[0, :, state.shape[2] - LANES :].astype(F32)
    return parts[0:1] + parts[1:2] + parts[2:3]


def log_rows(log):
    high, middle, low = split_in_three(log)
    return jnp.concatenate([high, middle, low, jnp.zeros((5, LANES), BF16)], axis=0)


def with_log(target, g, state, log):
    inner = target.shape[2] - LANES
    target[g, :, :inner] = state.astype(BF16)
    target[g, :, inner:] = log


def decay_rows(logs, inner):
    logs = logs + [jnp.zeros((1, LANES), F32)] * (8 - len(logs))
    return jnp.exp(over_channels(jnp.concatenate(logs, axis=0), head_lanes(inner)))


def chip_kernel(place, mine, got, *refs):
    parts, chip = refs[:-1], refs[-1]
    groups, _, width = mine.shape
    inner = width - LANES
    first = place[1] == 0
    log_mine, log_got = log_decay(mine), log_decay(got)
    later = decay_rows([jnp.where(first, log_got, log_mine)], inner)[0:1]
    log = log_rows(log_mine + log_got)
    for g in range(groups):
        a, b = mine[g, :, :inner].astype(F32), got[g, :, :inner].astype(F32)
        with_log(chip, g, later * jnp.where(first, a, b) + jnp.where(first, b, a), log)
    count = groups // len(parts)
    for d, part in enumerate(parts):
        part[...] = chip[pl.ds(lax.rem(place[2] + d, len(parts)) * count, count)]


def row_kernel(place, *refs):
    ways = (len(refs) - 4)
    parts, (row, before, logs, table) = refs[:ways], refs[ways:]
    count, _, width = row.shape
    inner = width - LANES
    for d, part in enumerate(parts):
        table[lax.rem(place[2] + ways - d, ways)] = part[...]
    each = [log_decay(table.at[k]) for k in range(ways)]
    decay = decay_rows(each, inner)
    total = jnp.zeros((1, LANES), F32)
    sums = []
    for k in range(ways):
        sums.append(total)
        total = total + each[k]
    logs[...] = jnp.concatenate(sums + [total] * (8 - ways), axis=0)
    log = log_rows(total)
    for g in range(count):
        state = jnp.zeros((8, inner), F32)
        for k in range(ways):
            before[k, g] = state
            state = decay[k : k + 1] * state + table[k, g, :, :inner].astype(F32)
        with_log(row, g, state, log)


def entering_kernel(place, before, logs, *refs):
    ways, count, _, inner = before.shape
    rows, parts, entering = refs[: ways - 1], refs[ways - 1 : -1], refs[-1]
    decay = decay_rows([log_decay(row) for row in rows], inner)
    inside = decay_rows([logs[k : k + 1, :] for k in range(ways)], inner)
    for g in range(count):
        state = jnp.zeros((8, inner), F32)
        for d in reversed(range(1, ways)):
            ahead = decay[d - 1 : d] * state + rows[d - 1][g, :, :inner].astype(F32)
            state = jnp.where(place[3] >= d, ahead, state)
        for k in range(ways):
            entering[k, g] = (before[k, g] + inside[k : k + 1] * state).astype(BF16)
    for d, part in enumerate(parts):
        part[...] = entering[lax.rem(place[2] + d, ways)]


def arrive_kernel(place, mine, got, *refs):
    parts, (own, give, whole) = refs[:-3], refs[-3:]
    ways = len(parts)
    groups, _, inner = whole.shape
    count = groups // ways
    for d, part in enumerate(parts):
        whole[pl.ds(lax.rem(place[2] + ways - d, ways) * count, count)] = part[...]
    first = place[1] == 0
    decay = decay_rows([jnp.where(first, log_decay(mine), log_decay(got))], inner)[0:1]
    for g in range(groups):
        state = whole[g].astype(F32)
        a, b = mine[g, :, :inner].astype(F32), got[g, :, :inner].astype(F32)
        after = decay * state + jnp.where(first, a, b)
        own[8 * g : 8 * g + 8, :] = jnp.where(first, state, after).astype(BF16)
        give[8 * g : 8 * g + 8, :] = jnp.where(first, after, state).astype(BF16)


def within_kernel(batch, length, b_rows, c_rows, starts, *refs):
    scaled, out = refs[:batch], refs[batch]
    blocks = length // BLOCK
    i = lax.broadcasted_iota(jnp.int32, (BLOCK, BLOCK), 0)
    j = lax.broadcasted_iota(jnp.int32, (BLOCK, BLOCK), 1)
    for b in range(batch):
        for k in range(blocks):
            n = b * blocks + k
            at = slice(k * BLOCK, (k + 1) * BLOCK)
            c = c_rows[n * BLOCK : (n + 1) * BLOCK, :]
            scores = dot(c, b_rows[b, :, at])
            scores = jnp.where(i >= j, scores, 0.0).astype(BF16)
            out[n * BLOCK : (n + 1) * BLOCK, :] = dot(scores, scaled[b][at, :]) + dot(c, starts[n])


def gated_kernel(batch, length, place, own, taken, within, c_rows, *refs):
    opened, refs = refs[:batch], refs[batch:]
    rows, (gated, squares, arrived) = refs[:batch], refs[batch:]
    blocks = length // BLOCK
    ones = jnp.ones((8, gated.shape[1]), BF16)
    arrived[place[1]] = own[...]
    arrived[1 - place[1]] = taken[...]
    for b in range(batch):
        for k in range(blocks):
            n = b * blocks + k
            at = slice(k * BLOCK, (k + 1) * BLOCK)
            token = slice(n * BLOCK, (n + 1) * BLOCK)
            late = dot(c_rows[token, :], arrived[b])
            y = within[token, :] + rows[b][blocks + k : blocks + k + 1, :] * late
            g = y * opened[b][at, :].astype(F32)
            gated[token, :] = g
            squares[:, n, :] = dot_nt(ones, (g * g).astype(BF16))


def scale_kernel(gated, squares, gain, out):
    total = squares[0]
    for d in range(1, squares.shape[0]):
        total = total + squares[d]
    scale = lax.rsqrt(total / DI + EPSILON)
    count = scale.shape[0]
    scale = jnp.concatenate([scale, jnp.zeros((LANES - count, LANES), F32)], axis=0)
    columns = jnp.transpose(scale)
    for n in range(count):
        at = slice(n * LANES, (n + 1) * LANES)
        out[at, :] = (gated[at, :] * columns[:, n : n + 1] * gain[...][None, :]).astype(BF16)


ANY = pl.BlockSpec(memory_space=pl.ANY)
WHOLE = pl.BlockSpec(memory_space=pltpu.VMEM)


def call(kernel, out, ins=None, scratch=(), mib=12, flops=0, outs=None, grid=()):
    shapes = [jax.ShapeDtypeStruct(s, d) for s, d in out]
    specs = {} if ins is None else {"in_specs": ins}
    if outs is not None:
        specs["out_specs"] = outs if len(outs) > 1 else outs[0]
    return pl.pallas_call(
        kernel,
        out_shape=shapes if len(shapes) > 1 else shapes[0],
        grid=grid,
        scratch_shapes=[s if not isinstance(s, tuple) else pltpu.VMEM(*s) for s in scratch],
        compiler_params=pltpu.CompilerParams(vmem_limit_bytes=mib << 20),
        cost_estimate=pl.CostEstimate(flops=flops, transcendentals=0, bytes_accessed=0)
        if flops
        else None,
        **specs,
    )


def on_device(
    hidden_in, gate_proj, value_proj, bc_proj, step_proj, value_conv, bc_conv, step_bias, log_rate,
    norm_gain,
):
    batch, length, width = hidden_in.shape
    tokens = batch * length
    inner = value_proj.shape[1]
    heads = step_proj.shape[1]
    share = bc_proj.shape[1]
    states = 2 * STATE
    blocks = tokens // BLOCK
    seq, tp = lax.axis_size("seq"), lax.axis_size("tp")
    hidden = hidden_in.reshape(tokens, width)
    weight = bc_proj.T
    step_weight = step_proj.T
    at = lax.axis_index("seq")
    place = jnp.stack([lax.axis_index("tp"), at % 2, at // 2 % WAYS, at // (2 * WAYS)])
    smem = pl.BlockSpec(memory_space=pltpu.SMEM)
    tail = hidden_in[:, length - 8 :, :]
    halo = lax.ppermute(tail, "seq", [(i, i + 1) for i in range(seq - 1)]).reshape(8 * batch, width)
    own, step_pre = call(
        functools.partial(bc_kernel, 256),
        [((share, tokens), BF16), ((tokens, LANES), F32)],
        scratch=[((256, LANES), F32), ((16 + share, width), BF16)],
        flops=6 * tokens * width * share,
    )(hidden, weight, step_weight)
    shard = call(
        functools.partial(join_kernel, batch),
        [((share, tokens + LANES), BF16)],
        scratch=[((LANES, LANES), F32)],
        flops=30 * tokens * width * share,
    )(halo, weight, own)
    work = 2 * length * width * inner

    def value_of(b, hidden):
        return call(
            functools.partial(value_kernel, b, length, heads),
            [
                ((length, inner), BF16),
                ((length, LANES), F32),
                ((2 * length // BLOCK, inner), F32),
                ((8, LANES), BF16),
            ],
            ins=[smem] * 2 + [WHOLE] * 5,
            outs=[WHOLE] * 4,
            scratch=[((length + 8, inner), F32)],
            flops=work,
        )(step_bias, log_rate, hidden, halo, value_proj, value_conv, step_pre)

    def gate_of(b, hidden, opening):
        return call(
            functools.partial(gate_kernel, b, length), [((length, inner), BF16)], flops=work
        )(hidden, gate_proj, opening)

    up = [(i, (i + 1) % tp) for i in range(tp)]
    down = [(i, (i - 1) % tp) for i in range(tp)]
    shards, places = [shard], [0]
    left = right = shard
    scaled, openings, rows, decays, opened = [], [], [], [], []
    for r in range(tp // 2):
        to_left = lax.ppermute(right, "tp", down) if 2 * r + 2 < tp else right
        to_right = lax.ppermute(left, "tp", up)
        if r < batch:
            one = value_of(r, hidden)
            for where, part in zip((scaled, openings, rows, decays), one):
                where.append(part)
            mark = one[3]
        elif r < 2 * batch:
            mark = gate_of(r - batch, hidden, openings[r - batch])
            opened.append(mark)
        left, right, hidden, mark = lax.optimization_barrier((to_right, to_left, hidden, mark))
        if r < batch:
            decays[-1] = mark
        else:
            opened[-1] = mark
        shards.append(left)
        places.append(tp - r - 1)
        if 2 * r + 2 < tp:
            shards.append(right)
            places.append(r + 1)
    group, quarter = STATE // 8, STATE // 8 // WAYS
    full = (group, 8, inner + LANES)
    part = (quarter, 8, inner + LANES)
    b_rows, c_rows, starts, mine, other = call(
        functools.partial(state_kernel, batch, length, places),
        [
            ((batch, STATE, length), BF16),
            ((tokens, STATE), BF16),
            ((blocks, STATE, inner), BF16),
            (full, BF16),
            (full, BF16),
        ],
        ins=[smem] + [WHOLE] * (1 + tp + 3 * batch),
        outs=[WHOLE] * 5,
        scratch=[((states, tokens), F32), ((states, LANES), F32)],
    )(place, bc_conv, *shards, *scaled, *rows, *decays)

    def to_core(x):
        return lax.ppermute(x, "seq", [(i, i ^ 1) for i in range(seq)])

    def along(x, step, stride):
        ring = stride * WAYS
        pairs = [(i, i // ring * ring + (i + step * stride) % ring) for i in range(seq)]
        return lax.ppermute(x, "seq", pairs)

    order = (1, WAYS - 1, *range(2, WAYS - 1))

    def hop(parts, stride):
        moved = {d: along(parts[d], d, stride) for d in order}
        return [moved[d] for d in range(1, WAYS)]

    got = to_core(other)
    leaving = call(
        chip_kernel,
        [(part, BF16)] * WAYS,
        ins=[smem, WHOLE, WHOLE],
        outs=[WHOLE] * WAYS,
        scratch=[(full, BF16)],
    )(place, mine, got)
    parts = hop(leaving, 2)
    row, before, logs = call(
        row_kernel,
        [(part, BF16), ((WAYS, quarter, 8, inner), F32), ((8, LANES), F32)],
        ins=[smem] + [WHOLE] * WAYS,
        outs=[WHOLE] * 3,
        scratch=[((WAYS,) + part, BF16)],
    )(place, leaving[0], *parts)
    row, starts = lax.optimization_barrier((row, starts))
    others = hop([row] * WAYS, 2 * WAYS)
    within = call(
        functools.partial(within_kernel, batch, length), [((tokens, inner), F32)], flops=work // 4
    )(b_rows, c_rows, starts, *scaled)
    *others, within = lax.optimization_barrier((*others, within))
    leaving = call(
        entering_kernel,
        [((quarter, 8, inner), BF16)] * WAYS,
        ins=[smem] + [WHOLE] * (1 + WAYS),
        outs=[WHOLE] * WAYS,
        scratch=[((WAYS, quarter, 8, inner), BF16)],
    )(place, before, logs, *others)
    parts = hop(leaving, 2)
    own, give = call(
        arrive_kernel,
        [((STATE, inner), BF16)] * 2,
        ins=[smem] + [WHOLE] * (2 + WAYS),
        outs=[WHOLE] * 2,
        scratch=[((group, 8, inner), BF16)],
    )(place, mine, got, leaving[0], *parts)
    taken = to_core(give)
    gated, squares = call(
        functools.partial(gated_kernel, batch, length),
        [((tokens, inner), F32), ((tp, blocks, LANES), F32)],
        ins=[smem] + [WHOLE] * (4 + 2 * batch),
        outs=[WHOLE] * 2,
        scratch=[((batch, STATE, inner), BF16)],
    )(place, own, taken, within, c_rows, *opened, *rows)
    whole = lax.all_to_all(squares, "tp", 0, 0, tiled=True)
    out = call(scale_kernel, [((tokens, inner), BF16)])(gated, whole, norm_gain)
    return out.reshape(batch, length, inner)


def solution(mesh):
    placed = (
        P(None, "seq", None),
        P(None, "tp"),
        P(None, "tp"),
        P(None, "tp"),
        P(None, "tp"),
        P(None, "tp"),
        P(),
        P("tp"),
        P("tp"),
        P("tp"),
    )
    return jax.shard_map(
        on_device, mesh=mesh, in_specs=placed, out_specs=P(None, "seq", "tp"), check_vma=False
    )
```

```python
import functools

import jax
import jax.numpy as jnp
from jax import lax
from jax.experimental import pallas as pl
from jax.experimental.pallas import tpu as pltpu
from jax.sharding import Mesh
from jax.sharding import PartitionSpec as P

DI = 5120
HEAD_DIM = 64
STATE = 128
CONV = 4
BLOCK = 128
WAYS = 4
LANES = 128
EPSILON = 1e-05

F32 = jnp.float32
BF16 = jnp.bfloat16
HIGHEST = lax.Precision.HIGHEST
NT = (((1,), (1,)), ((), ()))


def dot(a, b):
    return jnp.dot(a, b, preferred_element_type=F32)


def dot_nt(a, b):
    return lax.dot_general(a, b, NT, preferred_element_type=F32)


def silu(x):
    half = 0.5 * x
    return half + half * jnp.tanh(half)


def split_in_three(x):
    high = x.astype(BF16)
    rest = x - high.astype(F32)
    middle = rest.astype(BF16)
    return high, middle, (rest - middle.astype(F32)).astype(BF16)


def head_lanes(width):
    head = lax.broadcasted_iota(jnp.int32, (2 * LANES, width), 1) // HEAD_DIM
    row = lax.broadcasted_iota(jnp.int32, (2 * LANES, width), 0)
    return (head == lax.rem(row, LANES)).astype(BF16)


def over_channels(x, spread):
    high, middle, _ = split_in_three(x)
    return dot(jnp.concatenate([high, middle], axis=1), spread)


def prepare_kernel(weight, step_weight, joined):
    joined[...] = jnp.zeros_like(joined)
    joined[: step_weight.shape[0], :] = step_weight[...]
    joined[16:, :] = weight[...]


def bc_kernel(chunk, hidden, joined, out, steps, pad):
    both = joined.shape[0]
    pad[...] = jnp.zeros_like(pad)
    for r in range(0, hidden.shape[0], chunk):
        pad[:, :both] = dot_nt(hidden[r : r + chunk, :], joined[...])
        steps[r : r + chunk, :] = pad[...]
        out[:, r : r + chunk] = jnp.transpose(pad[...])[16:both].astype(BF16)


def join_kernel(batch, halo, weight, own, out, pad):
    share = out.shape[0]
    before = dot_nt(halo[...], weight[16:, :])
    pad[...] = jnp.zeros_like(pad)
    for b in range(batch):
        pad[LANES - 8 - 64 * b : LANES - 64 * b, :share] = before[8 * b : 8 * b + 8]
    out[:, :LANES] = jnp.transpose(pad[...])[:share].astype(BF16)
    out[:, LANES:] = own[...]


def value_kernel(
    b, length, heads, step_bias, log_rate, hidden, halo, weight, taps, steps_in,
    scaled, opening, rows, decays, padded,
):
    inner = weight.shape[1]
    spread = head_lanes(inner)
    lane = lax.broadcasted_iota(jnp.int32, (1, LANES), 1)
    bias, rate = jnp.zeros((1, LANES), F32), jnp.full((1, LANES), -1e30, F32)
    for h in range(heads):
        bias = jnp.where(lane == h, step_bias[h], bias)
        rate = jnp.where(lane == h, log_rate[h], rate)
    rate = jnp.exp(rate)
    own = slice(b * length, (b + 1) * length)
    both = jnp.concatenate([halo[...], hidden[own, :]], axis=0)
    first = halo.shape[0]
    both = dot(both, weight[...]).astype(BF16).astype(F32)
    padded[0:8, :] = both[8 * b : 8 * b + 8]
    padded[8:, :] = both[first:]
    step_pre = steps_in[own, :] + bias
    steps = jnp.maximum(step_pre, 0.0) + jnp.log1p(jnp.exp(-jnp.abs(step_pre)))
    width = 3 * BLOCK
    i = lax.broadcasted_iota(jnp.int32, (BLOCK, width), 0)
    j = lax.rem(lax.broadcasted_iota(jnp.int32, (BLOCK, width), 1), BLOCK)
    lower = (i >= j).astype(BF16)
    blocks = range(0, length, BLOCK)
    parts = split_in_three(-steps * rate)
    side = [jnp.concatenate([part[r : r + BLOCK] for r in blocks], axis=1) for part in parts]
    cumulative = dot(lower, jnp.concatenate(side, axis=0))
    half = 0.5 * cumulative[BLOCK - 1 : BLOCK, :]
    centered = cumulative - half
    ahead = jnp.exp(-centered)
    behind = jnp.exp(centered)
    ahead = jnp.concatenate([ahead[:, k * LANES : (k + 1) * LANES] for k in range(len(blocks))], axis=0)
    ahead = over_channels(ahead * steps, spread)
    total = jnp.zeros((1, LANES), F32)
    halves, offsets = [], []
    for k, r in enumerate(blocks):
        lanes = slice(k * LANES, (k + 1) * LANES)
        halves.append(half[:, lanes])
        offsets.append(total + half[:, lanes])
        total = total + 2.0 * half[:, lanes]
        value = sum(taps[t : t + 1, :] * padded[r + 5 + t : r + 5 + t + BLOCK, :] for t in range(CONV))
        scaled[r : r + BLOCK, :] = (silu(value) * ahead[r : r + BLOCK]).astype(BF16)
        opening[r : r + BLOCK, :] = behind[:, lanes]
    high, middle, low = split_in_three(total)
    decays[...] = jnp.concatenate([high, middle, low, jnp.zeros((5, LANES), BF16)], axis=0)
    rows[...] = jnp.exp(over_channels(jnp.concatenate(halves + offsets, axis=0), spread))


def gate_kernel(b, length, hidden, weight, opening, out):
    gate = dot(hidden[b * length : (b + 1) * length, :], weight[...]).astype(BF16).astype(F32)
    out[...] = (silu(gate) * over_channels(opening[...], head_lanes(weight.shape[1]))).astype(BF16)


def state_kernel(batch, length, steps, place, taps, *refs):
    shards, refs = refs[: len(steps)], refs[len(steps) :]
    scaled, refs = refs[:batch], refs[batch:]
    rows, refs = refs[:batch], refs[batch:]
    decays, (b_rows, c_rows, starts, mine, other, mixed, columns) = refs[:batch], refs[batch:]
    blocks = length // BLOCK
    inner = scaled[0].shape[1]
    share = shards[0].shape[0]
    rest = jnp.zeros((LANES - CONV, 2 * STATE), F32)
    columns[...] = jnp.transpose(jnp.concatenate([taps[...], rest], axis=0))
    for step, shard in zip(steps, shards):
        first = pl.multiple_of(lax.rem(place[0] + step, len(steps)) * share, share)
        tap = columns[pl.ds(first, share), :]
        halo = shard[:, :LANES].astype(F32)
        for b in range(batch):
            own = shard[:, LANES + b * length : LANES + (b + 1) * length].astype(F32)
            before = pltpu.roll(halo, 64 * b, 1) if b else halo
            padded = jnp.concatenate([before, own], axis=1)
            total = tap[:, CONV - 1 : CONV] * own
            for t in range(CONV - 1):
                total = total + tap[:, t : t + 1] * pltpu.roll(padded, CONV - 1 - t, 1)[:, LANES:]
            mixed[pl.ds(first, share), b * length : (b + 1) * length] = silu(total)
    ended = []
    for b in range(batch):
        own = slice(b * length, (b + 1) * length)
        b_t = mixed[:STATE, own].astype(BF16)
        b_rows[b] = b_t
        c_rows[own, :] = jnp.transpose(mixed[STATE:, own]).astype(BF16)
        state = jnp.zeros((STATE, inner), F32)
        for k in range(blocks):
            half = rows[b][k : k + 1, :]
            ready = half * state
            starts[b * blocks + k] = ready.astype(BF16)
            at = slice(k * BLOCK, (k + 1) * BLOCK)
            state = half * (ready + dot(b_t[:, at], scaled[b][at, :]))
        ended.append(state)
    first = place[1] == 0
    for target, (a, b) in ((mine, (0, 1)), (other, (1, 0))):
        log = jnp.where(first, decays[a][...].astype(F32), decays[b][...].astype(F32)).astype(BF16)
        for g in range(STATE // 8):
            at = slice(8 * g, 8 * g + 8)
            target[g, :, :inner] = jnp.where(first, ended[a][at], ended[b][at]).astype(BF16)
            target[g, :, inner:] = log


def log_decay(state):
    parts = state[0, :, state.shape[2] - LANES :].astype(F32)
    return parts[0:1] + parts[1:2] + parts[2:3]


def log_rows(log):
    high, middle, low = split_in_three(log)
    return jnp.concatenate([high, middle, low, jnp.zeros((5, LANES), BF16)], axis=0)


def with_log(target, g, state, log):
    inner = target.shape[2] - LANES
    target[g, :, :inner] = state.astype(BF16)
    target[g, :, inner:] = log


def decay_rows(logs, inner):
    logs = logs + [jnp.zeros((1, LANES), F32)] * (8 - len(logs))
    return jnp.exp(over_channels(jnp.concatenate(logs, axis=0), head_lanes(inner)))


def chip_kernel(place, mine, got, *refs):
    parts, chip = refs[:-1], refs[-1]
    groups, _, width = mine.shape
    inner = width - LANES
    first = place[1] == 0
    log_mine, log_got = log_decay(mine), log_decay(got)
    later = decay_rows([jnp.where(first, log_got, log_mine)], inner)[0:1]
    log = log_rows(log_mine + log_got)
    for g in range(groups):
        a, b = mine[g, :, :inner].astype(F32), got[g, :, :inner].astype(F32)
        with_log(chip, g, later * jnp.where(first, a, b) + jnp.where(first, b, a), log)
    count = groups // len(parts)
    for d, part in enumerate(parts):
        part[...] = chip[pl.ds(lax.rem(place[2] + d, len(parts)) * count, count)]


def row_kernel(place, *refs):
    ways = (len(refs) - 4)
    parts, (row, before, logs, table) = refs[:ways], refs[ways:]
    count, _, width = row.shape
    inner = width - LANES
    for d, part in enumerate(parts):
        table[lax.rem(place[2] + ways - d, ways)] = part[...]
    each = [log_decay(table.at[k]) for k in range(ways)]
    decay = decay_rows(each, inner)
    total = jnp.zeros((1, LANES), F32)
    sums = []
    for k in range(ways):
        sums.append(total)
        total = total + each[k]
    logs[...] = jnp.concatenate(sums + [total] * (8 - ways), axis=0)
    log = log_rows(total)
    for g in range(count):
        state = jnp.zeros((8, inner), F32)
        for k in range(ways):
            before[k, g] = state
            state = decay[k : k + 1] * state + table[k, g, :, :inner].astype(F32)
        with_log(row, g, state, log)


def entering_kernel(place, before, logs, *refs):
    ways, count, _, inner = before.shape
    rows, parts, entering = refs[: ways - 1], refs[ways - 1 : -1], refs[-1]
    decay = decay_rows([log_decay(row) for row in rows], inner)
    inside = decay_rows([logs[k : k + 1, :] for k in range(ways)], inner)
    for g in range(count):
        state = jnp.zeros((8, inner), F32)
        for d in reversed(range(1, ways)):
            ahead = decay[d - 1 : d] * state + rows[d - 1][g, :, :inner].astype(F32)
            state = jnp.where(place[3] >= d, ahead, state)
        for k in range(ways):
            entering[k, g] = (before[k, g] + inside[k : k + 1] * state).astype(BF16)
    for d, part in enumerate(parts):
        part[...] = entering[lax.rem(place[2] + d, ways)]


def arrive_kernel(place, mine, got, *refs):
    parts, (own, give, whole) = refs[:-3], refs[-3:]
    ways = len(parts)
    groups, _, inner = whole.shape
    count = groups // ways
    for d, part in enumerate(parts):
        whole[pl.ds(lax.rem(place[2] + ways - d, ways) * count, count)] = part[...]
    first = place[1] == 0
    decay = decay_rows([jnp.where(first, log_decay(mine), log_decay(got))], inner)[0:1]
    for g in range(groups):
        state = whole[g].astype(F32)
        a, b = mine[g, :, :inner].astype(F32), got[g, :, :inner].astype(F32)
        after = decay * state + jnp.where(first, a, b)
        own[8 * g : 8 * g + 8, :] = jnp.where(first, state, after).astype(BF16)
        give[8 * g : 8 * g + 8, :] = jnp.where(first, after, state).astype(BF16)


def within_kernel(batch, length, b_rows, c_rows, starts, *refs):
    scaled, out = refs[:batch], refs[batch]
    blocks = length // BLOCK
    i = lax.broadcasted_iota(jnp.int32, (BLOCK, BLOCK), 0)
    j = lax.broadcasted_iota(jnp.int32, (BLOCK, BLOCK), 1)
    for b in range(batch):
        for k in range(blocks):
            n = b * blocks + k
            at = slice(k * BLOCK, (k + 1) * BLOCK)
            c = c_rows[n * BLOCK : (n + 1) * BLOCK, :]
            scores = dot(c, b_rows[b, :, at])
            scores = jnp.where(i >= j, scores, 0.0).astype(BF16)
            out[n * BLOCK : (n + 1) * BLOCK, :] = dot(scores, scaled[b][at, :]) + dot(c, starts[n])


def gated_kernel(batch, length, place, own, taken, within, c_rows, *refs):
    opened, refs = refs[:batch], refs[batch:]
    rows, (gated, squares, arrived) = refs[:batch], refs[batch:]
    blocks = length // BLOCK
    ones = jnp.ones((8, gated.shape[1]), BF16)
    arrived[place[1]] = own[...]
    arrived[1 - place[1]] = taken[...]
    for b in range(batch):
        for k in range(blocks):
            n = b * blocks + k
            at = slice(k * BLOCK, (k + 1) * BLOCK)
            token = slice(n * BLOCK, (n + 1) * BLOCK)
            late = dot(c_rows[token, :], arrived[b])
            y = within[token, :] + rows[b][blocks + k : blocks + k + 1, :] * late
            g = y * opened[b][at, :].astype(F32)
            gated[token, :] = g
            squares[:, n, :] = dot_nt(ones, (g * g).astype(BF16))


def scale_kernel(gated, squares, gain, out):
    total = squares[0]
    for d in range(1, squares.shape[0]):
        total = total + squares[d]
    scale = lax.rsqrt(total / DI + EPSILON)
    count = scale.shape[0]
    scale = jnp.concatenate([scale, jnp.zeros((LANES - count, LANES), F32)], axis=0)
    columns = jnp.transpose(scale)
    for n in range(count):
        at = slice(n * LANES, (n + 1) * LANES)
        out[at, :] = (gated[at, :] * columns[:, n : n + 1] * gain[...][None, :]).astype(BF16)


ANY = pl.BlockSpec(memory_space=pl.ANY)
WHOLE = pl.BlockSpec(memory_space=pltpu.VMEM)


def call(kernel, out, ins=None, scratch=(), mib=12, flops=0, outs=None, grid=()):
    shapes = [jax.ShapeDtypeStruct(s, d) for s, d in out]
    specs = {} if ins is None else {"in_specs": ins}
    if outs is not None:
        specs["out_specs"] = outs if len(outs) > 1 else outs[0]
    return pl.pallas_call(
        kernel,
        out_shape=shapes if len(shapes) > 1 else shapes[0],
        grid=grid,
        scratch_shapes=[s if not isinstance(s, tuple) else pltpu.VMEM(*s) for s in scratch],
        compiler_params=pltpu.CompilerParams(vmem_limit_bytes=mib << 20),
        cost_estimate=pl.CostEstimate(flops=flops, transcendentals=0, bytes_accessed=0)
        if flops
        else None,
        **specs,
    )


def on_device(
    hidden_in, gate_proj, value_proj, bc_proj, step_proj, value_conv, bc_conv, step_bias, log_rate,
    norm_gain,
):
    batch, length, width = hidden_in.shape
    tokens = batch * length
    inner = value_proj.shape[1]
    heads = step_proj.shape[1]
    share = bc_proj.shape[1]
    states = 2 * STATE
    blocks = tokens // BLOCK
    seq, tp = lax.axis_size("seq"), lax.axis_size("tp")
    hidden = hidden_in.reshape(tokens, width)
    weight = bc_proj.T
    step_weight = step_proj.T
    at = lax.axis_index("seq")
    place = jnp.stack([lax.axis_index("tp"), at % 2, at // 2 % WAYS, at // (2 * WAYS)])
    smem = pl.BlockSpec(memory_space=pltpu.SMEM)
    joined = call(
        prepare_kernel, [((16 + share, width), BF16)], flops=20 * tokens * width * share
    )(weight, step_weight)
    tail = hidden_in[:, length - 8 :, :]
    tail, joined, place = lax.optimization_barrier((tail, joined, place))
    halo = lax.ppermute(tail, "seq", [(i, i + 1) for i in range(seq - 1)]).reshape(8 * batch, width)
    own, step_pre = call(
        functools.partial(bc_kernel, 256),
        [((share, tokens), BF16), ((tokens, LANES), F32)],
        scratch=[((256, LANES), F32)],
        flops=6 * tokens * width * share,
    )(hidden, joined)
    shard = call(
        functools.partial(join_kernel, batch),
        [((share, tokens + LANES), BF16)],
        scratch=[((LANES, LANES), F32)],
        flops=30 * tokens * width * share,
    )(halo, joined, own)
    work = 2 * length * width * inner

    def value_of(b, hidden):
        return call(
            functools.partial(value_kernel, b, length, heads),
            [
                ((length, inner), BF16),
                ((length, LANES), F32),
                ((2 * length // BLOCK, inner), F32),
                ((8, LANES), BF16),
            ],
            ins=[smem] * 2 + [WHOLE] * 5,
            outs=[WHOLE] * 4,
            scratch=[((length + 8, inner), F32)],
            flops=work,
        )(step_bias, log_rate, hidden, halo, value_proj, value_conv, step_pre)

    def gate_of(b, hidden, opening):
        return call(
            functools.partial(gate_kernel, b, length), [((length, inner), BF16)], flops=work
        )(hidden, gate_proj, opening)

    up = [(i, (i + 1) % tp) for i in range(tp)]
    down = [(i, (i - 1) % tp) for i in range(tp)]
    shards, places = [shard], [0]
    left = right = shard
    scaled, openings, rows, decays, opened = [], [], [], [], []
    for r in range(tp // 2):
        to_left = lax.ppermute(right, "tp", down) if 2 * r + 2 < tp else right
        to_right = lax.ppermute(left, "tp", up)
        if r < batch:
            one = value_of(r, hidden)
            for where, part in zip((scaled, openings, rows, decays), one):
                where.append(part)
            mark = one[3]
            left, right, hidden, mark = lax.optimization_barrier((to_right, to_left, hidden, mark))
            decays[-1] = mark
        else:
            left, right = to_right, to_left
        shards.append(left)
        places.append(tp - r - 1)
        if 2 * r + 2 < tp:
            shards.append(right)
            places.append(r + 1)
    group, quarter = STATE // 8, STATE // 8 // WAYS
    full = (group, 8, inner + LANES)
    part = (quarter, 8, inner + LANES)
    b_rows, c_rows, starts, mine, other = call(
        functools.partial(state_kernel, batch, length, places),
        [
            ((batch, STATE, length), BF16),
            ((tokens, STATE), BF16),
            ((blocks, STATE, inner), BF16),
            (full, BF16),
            (full, BF16),
        ],
        ins=[smem] + [WHOLE] * (1 + tp + 3 * batch),
        outs=[WHOLE] * 5,
        scratch=[((states, tokens), F32), ((states, LANES), F32)],
    )(place, bc_conv, *shards, *scaled, *rows, *decays)

    def to_core(x):
        return lax.ppermute(x, "seq", [(i, i ^ 1) for i in range(seq)])

    def along(x, step, stride):
        ring = stride * WAYS
        pairs = [(i, i // ring * ring + (i + step * stride) % ring) for i in range(seq)]
        return lax.ppermute(x, "seq", pairs)

    order = (1, WAYS - 1, *range(2, WAYS - 1))

    def hop(parts, stride):
        moved = {d: along(parts[d], d, stride) for d in order}
        return [moved[d] for d in range(1, WAYS)]

    def tie(x, after):
        return lax.optimization_barrier((x, after))[0]

    got = to_core(other)
    leaving = call(
        chip_kernel,
        [(part, BF16)] * WAYS,
        ins=[smem, WHOLE, WHOLE],
        outs=[WHOLE] * WAYS,
        scratch=[(full, BF16)],
    )(place, mine, got)
    parts = hop(leaving, 2)
    opened.append(gate_of(0, hidden, tie(openings[0], leaving[0])))
    *parts, opened[0] = lax.optimization_barrier((*parts, opened[0]))
    row, before, logs = call(
        row_kernel,
        [(part, BF16), ((WAYS, quarter, 8, inner), F32), ((8, LANES), F32)],
        ins=[smem] + [WHOLE] * WAYS,
        outs=[WHOLE] * 3,
        scratch=[((WAYS,) + part, BF16)],
    )(place, leaving[0], *parts)
    row, starts = lax.optimization_barrier((row, starts))
    others = hop([row] * WAYS, 2 * WAYS)
    within = call(
        functools.partial(within_kernel, batch, length), [((tokens, inner), F32)], flops=work // 4
    )(b_rows, c_rows, starts, *scaled)
    *others, within = lax.optimization_barrier((*others, within))
    leaving = call(
        entering_kernel,
        [((quarter, 8, inner), BF16)] * WAYS,
        ins=[smem] + [WHOLE] * (1 + WAYS),
        outs=[WHOLE] * WAYS,
        scratch=[((WAYS, quarter, 8, inner), BF16)],
    )(place, before, logs, *others)
    parts = hop(leaving, 2)
    opened.append(gate_of(1, hidden, tie(openings[1], leaving[0])))
    *parts, opened[1] = lax.optimization_barrier((*parts, opened[1]))
    own, give = call(
        arrive_kernel,
        [((STATE, inner), BF16)] * 2,
        ins=[smem] + [WHOLE] * (2 + WAYS),
        outs=[WHOLE] * 2,
        scratch=[((group, 8, inner), BF16)],
    )(place, mine, got, leaving[0], *parts)
    taken = to_core(give)
    gated, squares = call(
        functools.partial(gated_kernel, batch, length),
        [((tokens, inner), F32), ((tp, blocks, LANES), F32)],
        ins=[smem] + [WHOLE] * (4 + 2 * batch),
        outs=[WHOLE] * 2,
        scratch=[((batch, STATE, inner), BF16)],
    )(place, own, taken, within, c_rows, *opened, *rows)
    whole = lax.all_to_all(squares, "tp", 0, 0, tiled=True)
    out = call(scale_kernel, [((tokens, inner), BF16)])(gated, whole, norm_gain)
    return out.reshape(batch, length, inner)


def solution(mesh):
    placed = (
        P(None, "seq", None),
        P(None, "tp"),
        P(None, "tp"),
        P(None, "tp"),
        P(None, "tp"),
        P(None, "tp"),
        P(),
        P("tp"),
        P("tp"),
        P("tp"),
    )
    return jax.shard_map(
        on_device, mesh=mesh, in_specs=placed, out_specs=P(None, "seq", "tp"), check_vma=False
    )
```

```python
import functools

import jax
import jax.numpy as jnp
from jax import lax
from jax.experimental import pallas as pl
from jax.experimental.pallas import tpu as pltpu
from jax.sharding import Mesh
from jax.sharding import PartitionSpec as P

DI = 5120
HEAD_DIM = 64
STATE = 128
CONV = 4
BLOCK = 128
LANES = 128
EPSILON = 1e-05

F32 = jnp.float32
BF16 = jnp.bfloat16
HIGHEST = lax.Precision.HIGHEST
NT = (((1,), (1,)), ((), ()))


def dot(a, b):
    return jnp.dot(a, b, preferred_element_type=F32)


def dot_nt(a, b):
    return lax.dot_general(a, b, NT, preferred_element_type=F32)


def silu(x):
    half = 0.5 * x
    return half + half * jnp.tanh(half)


def split_in_three(x):
    high = x.astype(BF16)
    rest = x - high.astype(F32)
    middle = rest.astype(BF16)
    return high, middle, (rest - middle.astype(F32)).astype(BF16)


def head_lanes(width):
    head = lax.broadcasted_iota(jnp.int32, (2 * LANES, width), 1) // HEAD_DIM
    row = lax.broadcasted_iota(jnp.int32, (2 * LANES, width), 0)
    return (head == lax.rem(row, LANES)).astype(BF16)


def over_channels(x, spread):
    high, middle, _ = split_in_three(x)
    return dot(jnp.concatenate([high, middle], axis=1), spread)


def tail_kernel(batch, length, hidden, out):
    for b in range(batch):
        out[8 * b : 8 * b + 8, :] = hidden[(b + 1) * length - 8 : (b + 1) * length, :]


def bc_kernel(chunk, hidden, weight, step_weight, out, steps, pad, joined):
    share = weight.shape[0]
    joined[...] = jnp.zeros_like(joined)
    joined[: step_weight.shape[0], :] = step_weight[...]
    joined[16 : 16 + share, :] = weight[...]
    pad[...] = jnp.zeros_like(pad)
    for r in range(0, hidden.shape[0], chunk):
        pad[:, : 16 + share] = dot_nt(hidden[r : r + chunk, :], joined[...])
        steps[r : r + chunk, :] = pad[...]
        out[:, r : r + chunk] = jnp.transpose(pad[...])[16 : 16 + share].astype(BF16)


def join_kernel(batch, halo, weight, own, out, pad):
    share = weight.shape[0]
    before = dot_nt(halo[...], weight[...])
    pad[...] = jnp.zeros_like(pad)
    for b in range(batch):
        pad[LANES - 8 - 64 * b : LANES - 64 * b, :share] = before[8 * b : 8 * b + 8]
    out[:, :LANES] = jnp.transpose(pad[...])[:share].astype(BF16)
    out[:, LANES:] = own[...]


def value_kernel(
    b, length, heads, step_bias, log_rate, hidden, halo, weight, taps, steps_in,
    scaled, opening, rows, decays, padded,
):
    inner = weight.shape[1]
    spread = head_lanes(inner)
    lane = lax.broadcasted_iota(jnp.int32, (1, LANES), 1)
    bias, rate = jnp.zeros((1, LANES), F32), jnp.full((1, LANES), -1e30, F32)
    for h in range(heads):
        bias = jnp.where(lane == h, step_bias[h], bias)
        rate = jnp.where(lane == h, log_rate[h], rate)
    rate = jnp.exp(rate)
    own = slice(b * length, (b + 1) * length)
    both = jnp.concatenate([halo[...], hidden[own, :]], axis=0)
    first = halo.shape[0]
    both = dot(both, weight[...]).astype(BF16).astype(F32)
    padded[0:8, :] = both[8 * b : 8 * b + 8]
    padded[8:, :] = both[first:]
    step_pre = steps_in[own, :] + bias
    steps = jnp.maximum(step_pre, 0.0) + jnp.log1p(jnp.exp(-jnp.abs(step_pre)))
    width = 3 * BLOCK
    i = lax.broadcasted_iota(jnp.int32, (BLOCK, width), 0)
    j = lax.rem(lax.broadcasted_iota(jnp.int32, (BLOCK, width), 1), BLOCK)
    lower = (i >= j).astype(BF16)
    blocks = range(0, length, BLOCK)
    parts = split_in_three(-steps * rate)
    side = [jnp.concatenate([part[r : r + BLOCK] for r in blocks], axis=1) for part in parts]
    cumulative = dot(lower, jnp.concatenate(side, axis=0))
    half = 0.5 * cumulative[BLOCK - 1 : BLOCK, :]
    centered = cumulative - half
    ahead = jnp.exp(-centered)
    behind = jnp.exp(centered)
    ahead = jnp.concatenate([ahead[:, k * LANES : (k + 1) * LANES] for k in range(len(blocks))], axis=0)
    ahead = over_channels(ahead * steps, spread)
    total = jnp.zeros((1, LANES), F32)
    halves, offsets = [], []
    for k, r in enumerate(blocks):
        lanes = slice(k * LANES, (k + 1) * LANES)
        halves.append(half[:, lanes])
        offsets.append(total + half[:, lanes])
        total = total + 2.0 * half[:, lanes]
        value = sum(taps[t : t + 1, :] * padded[r + 5 + t : r + 5 + t + BLOCK, :] for t in range(CONV))
        scaled[r : r + BLOCK, :] = (silu(value) * ahead[r : r + BLOCK]).astype(BF16)
        opening[r : r + BLOCK, :] = behind[:, lanes]
    high, middle, low = split_in_three(total)
    decays[...] = jnp.concatenate([high, middle, low, jnp.zeros((5, LANES), BF16)], axis=0)
    rows[...] = jnp.exp(over_channels(jnp.concatenate(halves + offsets, axis=0), spread))


def gate_kernel(b, length, hidden, weight, opening, out):
    gate = dot(hidden[b * length : (b + 1) * length, :], weight[...]).astype(BF16).astype(F32)
    out[...] = (silu(gate) * over_channels(opening[...], head_lanes(weight.shape[1]))).astype(BF16)


def state_kernel(batch, length, steps, place, taps, *refs):
    shards, refs = refs[: len(steps)], refs[len(steps) :]
    scaled, refs = refs[:batch], refs[batch:]
    rows, refs = refs[:batch], refs[batch:]
    decays, (b_rows, c_rows, starts, sent, mixed, columns) = refs[:batch], refs[batch:]
    blocks = length // BLOCK
    inner = scaled[0].shape[1]
    share = shards[0].shape[0]
    rest = jnp.zeros((LANES - CONV, 2 * STATE), F32)
    columns[...] = jnp.transpose(jnp.concatenate([taps[...], rest], axis=0))
    for step, shard in zip(steps, shards):
        first = pl.multiple_of(lax.rem(place[0] + step, len(steps)) * share, share)
        tap = columns[pl.ds(first, share), :]
        halo = shard[:, :LANES].astype(F32)
        for b in range(batch):
            own = shard[:, LANES + b * length : LANES + (b + 1) * length].astype(F32)
            before = pltpu.roll(halo, 64 * b, 1) if b else halo
            padded = jnp.concatenate([before, own], axis=1)
            total = tap[:, CONV - 1 : CONV] * own
            for t in range(CONV - 1):
                total = total + tap[:, t : t + 1] * pltpu.roll(padded, CONV - 1 - t, 1)[:, LANES:]
            mixed[pl.ds(first, share), b * length : (b + 1) * length] = silu(total)
    for b in range(batch):
        own = slice(b * length, (b + 1) * length)
        b_t = mixed[:STATE, own].astype(BF16)
        b_rows[b] = b_t
        c_rows[own, :] = jnp.transpose(mixed[STATE:, own]).astype(BF16)
        state = jnp.zeros((STATE, inner), F32)
        for k in range(blocks):
            half = rows[b][k : k + 1, :]
            ready = half * state
            starts[b * blocks + k] = ready.astype(BF16)
            at = slice(k * BLOCK, (k + 1) * BLOCK)
            state = half * (ready + dot(b_t[:, at], scaled[b][at, :]))
        for g in range(STATE // 8):
            sent[b, g, :, :inner] = state[8 * g : 8 * g + 8].astype(BF16)
            sent[b, g, :, inner:] = decays[b][...]


def scan_kernel(got, out, table, logs):
    devices, _, width = got.shape
    inner = width - LANES
    for s in range(devices):
        parts = got[s, :, inner:].astype(F32)
        table[s : s + 1, :] = parts[0:1] + parts[1:2] + parts[2:3]
    logs[...] = jnp.exp(over_channels(table[...], head_lanes(inner)))
    state = jnp.zeros((8, inner), F32)
    for s in range(devices):
        out[s] = state.astype(BF16)
        state = logs[s : s + 1, :] * state + got[s, :, :inner].astype(F32)


def gated_kernel(batch, length, arrived, b_rows, c_rows, starts, *refs):
    scaled, refs = refs[:batch], refs[batch:]
    opened, refs = refs[:batch], refs[batch:]
    rows, (gated, squares) = refs[:batch], refs[batch:]
    blocks = length // BLOCK
    ones = jnp.ones((8, gated.shape[1]), BF16)
    i = lax.broadcasted_iota(jnp.int32, (BLOCK, BLOCK), 0)
    j = lax.broadcasted_iota(jnp.int32, (BLOCK, BLOCK), 1)
    for b in range(batch):
        for k in range(blocks):
            n = b * blocks + k
            at = slice(k * BLOCK, (k + 1) * BLOCK)
            c = c_rows[n * BLOCK : (n + 1) * BLOCK, :]
            scores = dot(c, b_rows[b, :, at])
            scores = jnp.where(i >= j, scores, 0.0).astype(BF16)
            y = dot(scores, scaled[b][at, :]) + dot(c, starts[n])
            y = y + rows[b][blocks + k : blocks + k + 1, :] * dot(c, arrived[b])
            g = y * opened[b][at, :].astype(F32)
            gated[n * BLOCK : (n + 1) * BLOCK, :] = g
            squares[:, n, :] = dot_nt(ones, (g * g).astype(BF16))


def scale_kernel(gated, squares, gain, out):
    total = squares[0]
    for d in range(1, squares.shape[0]):
        total = total + squares[d]
    scale = lax.rsqrt(total / DI + EPSILON)
    count = scale.shape[0]
    scale = jnp.concatenate([scale, jnp.zeros((LANES - count, LANES), F32)], axis=0)
    columns = jnp.transpose(scale)
    for n in range(count):
        at = slice(n * LANES, (n + 1) * LANES)
        out[at, :] = (gated[at, :] * columns[:, n : n + 1] * gain[...][None, :]).astype(BF16)


ANY = pl.BlockSpec(memory_space=pl.ANY)
WHOLE = pl.BlockSpec(memory_space=pltpu.VMEM)


def call(kernel, out, ins=None, scratch=(), mib=12, flops=0, outs=None, grid=()):
    shapes = [jax.ShapeDtypeStruct(s, d) for s, d in out]
    specs = {} if ins is None else {"in_specs": ins}
    if outs is not None:
        specs["out_specs"] = outs if len(outs) > 1 else outs[0]
    return pl.pallas_call(
        kernel,
        out_shape=shapes if len(shapes) > 1 else shapes[0],
        grid=grid,
        scratch_shapes=[s if not isinstance(s, tuple) else pltpu.VMEM(*s) for s in scratch],
        compiler_params=pltpu.CompilerParams(vmem_limit_bytes=mib << 20),
        cost_estimate=pl.CostEstimate(flops=flops, transcendentals=0, bytes_accessed=0)
        if flops
        else None,
        **specs,
    )


def on_device(
    hidden_in, gate_proj, value_proj, bc_proj, step_proj, value_conv, bc_conv, step_bias, log_rate,
    norm_gain,
):
    batch, length, width = hidden_in.shape
    tokens = batch * length
    inner = value_proj.shape[1]
    heads = step_proj.shape[1]
    share = bc_proj.shape[1]
    states = 2 * STATE
    blocks = tokens // BLOCK
    seq, tp = lax.axis_size("seq"), lax.axis_size("tp")
    hidden = hidden_in.reshape(tokens, width)
    weight = bc_proj.T
    step_weight = step_proj.T
    place = lax.axis_index("tp").reshape(1)
    smem = pl.BlockSpec(memory_space=pltpu.SMEM)
    hidden, place = lax.optimization_barrier((hidden, place))
    tail = call(
        functools.partial(tail_kernel, batch, length),
        [((8 * batch, width), BF16)],
        flops=1 * tokens * width * share,
    )(hidden)
    halo = lax.ppermute(tail, "seq", [(i, i + 1) for i in range(seq - 1)])
    own, step_pre = call(
        functools.partial(bc_kernel, 256),
        [((share, tokens), BF16), ((tokens, LANES), F32)],
        scratch=[((256, LANES), F32), ((16 + share, width), BF16)],
        flops=6 * tokens * width * share,
    )(hidden, weight, step_weight)
    shard = call(
        functools.partial(join_kernel, batch),
        [((share, tokens + LANES), BF16)],
        scratch=[((LANES, LANES), F32)],
        flops=30 * tokens * width * share,
    )(halo, weight, own)
    work = 2 * length * width * inner

    def value_of(b, hidden):
        return call(
            functools.partial(value_kernel, b, length, heads),
            [
                ((length, inner), BF16),
                ((length, LANES), F32),
                ((2 * length // BLOCK, inner), F32),
                ((8, LANES), BF16),
            ],
            ins=[smem] * 2 + [WHOLE] * 5,
            outs=[WHOLE] * 4,
            scratch=[((length + 8, inner), F32)],
            flops=work,
        )(step_bias, log_rate, hidden, halo, value_proj, value_conv, step_pre)

    def gate_of(b, hidden, opening):
        return call(
            functools.partial(gate_kernel, b, length), [((length, inner), BF16)], flops=work
        )(hidden, gate_proj, opening)

    up = [(i, (i + 1) % tp) for i in range(tp)]
    down = [(i, (i - 1) % tp) for i in range(tp)]
    shards, places = [shard], [0]
    left = right = shard
    scaled, openings, rows, decays, opened = [], [], [], [], []
    for r in range(tp // 2):
        to_left = lax.ppermute(right, "tp", down) if 2 * r + 2 < tp else right
        to_right = lax.ppermute(left, "tp", up)
        if r < batch:
            one = value_of(r, hidden)
            for where, part in zip((scaled, openings, rows, decays), one):
                where.append(part)
            mark = one[3]
        elif r < 2 * batch:
            mark = gate_of(r - batch, hidden, openings[r - batch])
            opened.append(mark)
        left, right, hidden, mark = lax.optimization_barrier((to_right, to_left, hidden, mark))
        if r < batch:
            decays[-1] = mark
        else:
            opened[-1] = mark
        shards.append(left)
        places.append(tp - r - 1)
        if 2 * r + 2 < tp:
            shards.append(right)
            places.append(r + 1)
    b_rows, c_rows, starts, sent = call(
        functools.partial(state_kernel, batch, length, places),
        [
            ((batch, STATE, length), BF16),
            ((tokens, STATE), BF16),
            ((blocks, STATE, inner), BF16),
            ((batch, STATE // 8, 8, inner + LANES), BF16),
        ],
        ins=[smem] + [WHOLE] * (1 + tp + 3 * batch),
        outs=[WHOLE] * 4,
        scratch=[((states, tokens), F32), ((states, LANES), F32)],
    )(place, bc_conv, *shards, *scaled, *rows, *decays)
    got = lax.all_to_all(sent.reshape(seq, -1, inner + LANES), "seq", 0, 0, tiled=True)
    prefix = call(
        scan_kernel,
        [((seq, 8, inner), BF16)],
        scratch=[((seq, LANES), F32), ((seq, inner), F32)],
    )(got)
    arrived = lax.all_to_all(prefix, "seq", 0, 0, tiled=True).reshape(batch, STATE, inner)
    gated, squares = call(
        functools.partial(gated_kernel, batch, length),
        [((tokens, inner), F32), ((tp, blocks, LANES), F32)],
    )(arrived, b_rows, c_rows, starts, *scaled, *opened, *rows)
    whole = lax.all_to_all(squares, "tp", 0, 0, tiled=True)
    out = call(scale_kernel, [((tokens, inner), BF16)])(gated, whole, norm_gain)
    return out.reshape(batch, length, inner)


def solution(mesh):
    placed = (
        P(None, "seq", None),
        P(None, "tp"),
        P(None, "tp"),
        P(None, "tp"),
        P(None, "tp"),
        P(None, "tp"),
        P(),
        P("tp"),
        P("tp"),
        P("tp"),
    )
    return jax.shard_map(
        on_device, mesh=mesh, in_specs=placed, out_specs=P(None, "seq", "tp"), check_vma=False
    )
```
